32 devices in a mesh: grp: 4 (over z), dp: 2 (over x), tp: 4 (over y, core).
Axes of the slice: x: 2, y: 2, z: 4, core: 2. Of those that a mesh axis runs over, the one named last changes fastest.
Arguments:
- hidden_last: bfloat16 [128, 5120], P(('grp', 'dp')), may hold values from -6 to 6
- gain: float32 [5120], replicated, may hold values from 0.25 to 1.75
- w_query: bfloat16 [5120, 2560], P('dp', 'tp'), may hold values from -0.078125 to 0.078125
- w_key: bfloat16 [5120, 512], P('dp', 'tp'), may hold values from -0.078125 to 0.078125
- w_value: bfloat16 [5120, 512], P('dp', 'tp'), may hold values from -0.078125 to 0.078125
- w_out: bfloat16 [2560, 5120], P('tp'), may hold values from -0.125 to 0.125
- cache_keys: bfloat16 [128, 128, 512], P(('grp', 'dp'), None, 'tp'), may hold values from -6 to 6
- cache_values: bfloat16 [128, 128, 512], P(('grp', 'dp'), None, 'tp'), may hold values from -6 to 6
- cache_lengths: int32 [128], P(('grp', 'dp')), may hold values from 1 to 128
- reward_vec: float32 [5120], replicated, may hold values from -0.078125 to 0.078125
- response_counts: int32 [128], P('grp'), may hold values from 4 to 16
- assignment: int32 [128], P('grp'), may hold values from 0 to 1, as said below
- responses: bfloat16 [128, 16, 5120], P(('grp', 'dp'), None, 'tp'), may hold values from -6 to 6
- cotangent: bfloat16 [128, 16, 5120], P(('grp', 'dp'), None, 'tp'), may hold values from -6 to 6
Outputs:
- decoded: bfloat16 [128, 5120], P(('grp', 'dp'))
- advantage: float32 [128], P(('grp', 'dp'))
- layer_out: bfloat16 [128, 16, 5120], P(('grp', 'dp'), None, 'tp')
- grad_query: float32 [5120, 2560], P('dp', 'tp')
- grad_key: float32 [5120, 512], P('dp', 'tp')
- grad_value: float32 [5120, 512], P('dp', 'tp')
The draws below stay inside these ranges and needn't reach their ends.
Inputs may be any that keep to these rules, and one draw needn't show every extreme that they name: `assignment`: within each group, every training shard receives exactly 16 rows, and from the 16 rows of one device at most 10 rows go to one training shard; that most is reached for some shard in every group.
All inputs are finite; a program needn't handle non-finite values.
Results may differ from the reference program's by a relative error of at most 0.025.
Values may be sent and summed in bfloat16 or wider, within the bound.
A program may use at most 128 MiB of HBM per device.

```python
import jax
import jax.numpy as jnp
from jax import lax

D = 5120
HEADS = 20
KV_HEADS = 4
HEAD_DIM = 128
STEPS = 2
R_DEV = 16
CACHE = 128
MAXRESP = 16
GROUP_ROWS = 32
ROWS = 128
N_DP = 2
N_TP = 4


def draw_assignment(key, part):
    shards = GROUP_ROWS // R_DEV
    groups = ROWS // GROUP_ROWS
    base = R_DEV // shards

    def one_group(group_key):
        first_key, second_key = jax.random.split(group_key)
        first = jax.random.permutation(first_key, shards)
        second = jnp.roll(first, -1)
        columns = jnp.arange(shards)
        loads = base + 2 * (columns[None, :] == first[:, None]).astype(jnp.int32) - 2 * (columns[None, :] == second[:, None]).astype(jnp.int32)
        ends = jnp.cumsum(loads, axis=1)
        place = jnp.arange(R_DEV)
        target = jnp.sum((place[None, :, None] >= ends[:, None, :]).astype(jnp.int32), axis=2)
        row_keys = jax.random.split(second_key, shards)
        shuffled = jax.vmap(lambda row_key, row: jax.random.permutation(row_key, row))(row_keys, target)
        return shuffled.reshape(-1)
    group_keys = jax.random.split(jax.random.fold_in(key, 11), groups)
    return jax.vmap(one_group)(group_keys).reshape(-1).astype(jnp.int32)


def set_ends(array, rng, low, high):
    longest = array.shape.index(max(array.shape))
    spots = []
    for shift in (0, 1):
        where = [jax.random.randint(jax.random.fold_in(rng, axis), (), 0, length) for axis, length in enumerate(array.shape)]
        where[longest] = (where[longest] + shift) % array.shape[longest]
        spots.append(tuple(where))
    return array.at[spots[0]].set(low).at[spots[1]].set(high)


def levels(own_key, shape, cuts, smallest, largest):
    loudness = 1.0
    for axis_at, shards_of in cuts:
        steps = jax.random.uniform(jax.random.fold_in(jax.random.fold_in(own_key, 6), axis_at), (shards_of,), jnp.float32, smallest / len(cuts), largest / len(cuts))
        loudness = loudness * jnp.repeat(jnp.exp(steps), shape[axis_at] // shards_of).reshape((-1,) + (1,) * (len(shape) - 1 - axis_at))
    return loudness


def noise(rng, shape, width, bound, pieces=(), kind=jnp.bfloat16):
    result = width * jax.random.normal(rng, shape, jnp.float32)
    if pieces:
        result = result * levels(rng, shape, pieces, -0.22, 0.18)
    return jnp.clip(result, -bound, bound).astype(kind)


def setup_inputs(seed: int = 0) -> dict:
    streams_of = jax.random.split(jax.random.key(seed), 15)
    return {
        "hidden_last": noise(streams_of[0], (ROWS, D), 1.0, 6.0, ((0, 8),)),
        "gain": jnp.clip(1.0 + 0.15 * jax.random.normal(streams_of[1], (D,), jnp.float32), 0.25, 1.75),
        "w_query": noise(streams_of[2], (D, HEADS * HEAD_DIM), D ** -0.5, 0.078125, ((0, 2), (1, 4))),
        "w_key": noise(streams_of[3], (D, KV_HEADS * HEAD_DIM), D ** -0.5, 0.078125, ((0, 2), (1, 4))),
        "w_value": noise(streams_of[4], (D, KV_HEADS * HEAD_DIM), D ** -0.5, 0.078125, ((0, 2), (1, 4))),
        "w_out": noise(streams_of[5], (HEADS * HEAD_DIM, D), (HEADS * HEAD_DIM) ** -0.5, 0.125, ((0, 4),)),
        "cache_keys": noise(streams_of[6], (ROWS, CACHE, KV_HEADS * HEAD_DIM), 1.0, 6.0, ((0, 8), (2, 4))),
        "cache_values": noise(streams_of[7], (ROWS, CACHE, KV_HEADS * HEAD_DIM), 1.0, 6.0, ((0, 8), (2, 4))),
        "cache_lengths": set_ends(jax.random.randint(streams_of[8], (ROWS,), 1, CACHE + 1), jax.random.fold_in(streams_of[8], 1), 1, CACHE).astype(jnp.int32),
        "reward_vec": noise(streams_of[9], (D,), D ** -0.5, 0.078125, (), jnp.float32),
        "response_counts": set_ends(jax.random.randint(streams_of[10], (ROWS,), MAXRESP // 4, MAXRESP + 1), jax.random.fold_in(streams_of[10], 1), MAXRESP // 4, MAXRESP).astype(jnp.int32),
        "assignment": draw_assignment(jax.random.fold_in(streams_of[14], 71), 0),
        "responses": noise(streams_of[12], (ROWS, MAXRESP, D), 1.0, 6.0, ((0, 8), (2, 4))),
        "cotangent": noise(streams_of[13], (ROWS, MAXRESP, D), 1.0, 6.0, ((0, 8), (2, 4))),
    }


def norm_rows(values, gain):
    wide = values.astype(jnp.float32)
    meansq = lax.optimization_barrier(jnp.mean(wide * wide, axis=-1, keepdims=True))
    return (wide * lax.rsqrt(meansq + 1e-06) * gain).astype(jnp.bfloat16)

def rounded(values):
    return lax.optimization_barrier(values.astype(jnp.bfloat16)).astype(jnp.float32)

def decode_attend(query, cache_k, cache_v, lengths, new_k, new_v):
    rows_n = query.shape[0]
    slots = cache_k.shape[1]
    kv_n = cache_k.shape[2] // HEAD_DIM
    per_kv = query.shape[1] // cache_k.shape[2]
    scale = 1.0 / HEAD_DIM ** 0.5
    quer = query.reshape(rows_n, kv_n, per_kv, HEAD_DIM).astype(jnp.float32)
    keys_c = cache_k.reshape(rows_n, slots, kv_n, HEAD_DIM).astype(jnp.float32)
    vals_c = cache_v.reshape(rows_n, slots, kv_n, HEAD_DIM).astype(jnp.float32)
    keys_n = new_k.reshape(rows_n, -1, kv_n, HEAD_DIM).astype(jnp.float32)
    vals_n = new_v.reshape(rows_n, -1, kv_n, HEAD_DIM).astype(jnp.float32)
    score_c = jnp.einsum('rkgd,rckd->rkgc', quer, keys_c) * scale
    score_n = jnp.einsum('rkgd,rnkd->rkgn', quer, keys_n) * scale
    live = (jnp.arange(slots, dtype=jnp.int32)[None, :] < lengths[:, None])[:, None, None, :]
    score_c = jnp.where(live, score_c, -1e+30)
    scores = jnp.concatenate([score_c, score_n], axis=-1)
    expo = jnp.exp(scores)
    weights = (expo / lax.optimization_barrier(jnp.sum(expo, axis=-1, keepdims=True))).astype(jnp.bfloat16).astype(jnp.float32)
    context = jnp.einsum('rkgc,rckd->rkgd', weights[..., :slots], vals_c)
    context = context + jnp.einsum('rkgn,rnkd->rkgd', weights[..., slots:], vals_n)
    return context.reshape(rows_n, -1).astype(jnp.bfloat16)

def attend(query, keys, values, counts):
    rows_n = counts.shape[0]
    tokens = query.shape[0]
    length = tokens // rows_n
    kv_n = keys.shape[1] // HEAD_DIM
    per_kv = query.shape[1] // keys.shape[1]
    scale = 1.0 / HEAD_DIM ** 0.5
    quer = query.reshape(rows_n, length, kv_n, per_kv, HEAD_DIM).astype(jnp.float32)
    keyf = keys.reshape(rows_n, length, kv_n, HEAD_DIM).astype(jnp.float32)
    valf = values.reshape(rows_n, length, kv_n, HEAD_DIM).astype(jnp.float32)
    scores = jnp.einsum('rikgd,rjkd->rkgij', quer, keyf) * scale
    slot = jnp.arange(length, dtype=jnp.int32)
    causal = (slot[None, :] <= slot[:, None])[None, :, :]
    inside = slot[None, None, :] < counts[:, None, None]
    mask = (causal & inside)[:, None, None, :, :]
    scores = jnp.where(mask, scores, -1e+30)
    expo = jnp.exp(scores)
    weights = (expo / lax.optimization_barrier(jnp.sum(expo, axis=-1, keepdims=True))).astype(jnp.bfloat16).astype(jnp.float32)
    context = jnp.einsum('rkgij,rjkd->rikgd', weights, valf)
    return context.reshape(tokens, -1).astype(jnp.bfloat16)

def slot_valid(counts, length):
    slot = jnp.arange(length, dtype=jnp.int32)
    return (slot[None, :] < counts[:, None]).reshape(-1)

def reference(hidden_last, gain, w_query, w_key, w_value, w_out, cache_keys, cache_values, cache_lengths, reward_vec, response_counts, assignment, responses, cotangent):
    state = hidden_last
    keys_new = []
    values_new = []
    for step in range(STEPS):
        normed = norm_rows(state, gain)
        query = jnp.dot(normed, w_query, preferred_element_type=jnp.float32).astype(jnp.bfloat16)
        keys_new.append(jnp.dot(normed, w_key, preferred_element_type=jnp.float32).astype(jnp.bfloat16))
        values_new.append(jnp.dot(normed, w_value, preferred_element_type=jnp.float32).astype(jnp.bfloat16))
        context = decode_attend(query, cache_keys, cache_values, cache_lengths, jnp.stack(keys_new, 1), jnp.stack(values_new, 1))
        output = jnp.dot(context, w_out, preferred_element_type=jnp.float32)
        state = (state.astype(jnp.float32) + output).astype(jnp.bfloat16)
    reward = lax.optimization_barrier(jnp.sum(state.astype(jnp.float32) * reward_vec, axis=-1))
    grouped = reward.reshape(-1, GROUP_ROWS)
    mean = lax.optimization_barrier(jnp.sum(grouped, axis=1, keepdims=True)) / GROUP_ROWS
    spread = lax.optimization_barrier(jnp.sum(grouped * grouped, axis=1, keepdims=True)) / GROUP_ROWS - mean * mean
    advantage = ((grouped - mean) / jnp.sqrt(spread + 1e-05)).reshape(-1)
    adv_short = advantage.astype(jnp.bfloat16)
    head_cols = HEADS * HEAD_DIM // N_TP
    tokens = R_DEV * MAXRESP

    def shard_step(carry, shard):
        group = shard // N_DP
        index = shard % N_DP
        group_assign = lax.dynamic_slice_in_dim(assignment, (group * GROUP_ROWS).astype(jnp.int32), GROUP_ROWS)
        order = jnp.argsort(group_assign * GROUP_ROWS + jnp.arange(GROUP_ROWS, dtype=jnp.int32), stable=True).astype(jnp.int32)
        chosen = lax.dynamic_slice_in_dim(order, (index * R_DEV).astype(jnp.int32), R_DEV) + (group * GROUP_ROWS).astype(jnp.int32)
        inputs = jnp.take(responses, chosen, axis=0).reshape(tokens, D)
        counts = jnp.take(response_counts, chosen)
        weight_row = jnp.take(adv_short, chosen).astype(jnp.float32)
        upstream_raw = lax.dynamic_slice_in_dim(cotangent, (shard * R_DEV).astype(jnp.int32), R_DEV).reshape(tokens, D)
        normed = norm_rows(inputs, gain)
        query = jnp.dot(normed, w_query, preferred_element_type=jnp.float32).astype(jnp.bfloat16)
        keys = jnp.dot(normed, w_key, preferred_element_type=jnp.float32).astype(jnp.bfloat16)
        values = jnp.dot(normed, w_value, preferred_element_type=jnp.float32).astype(jnp.bfloat16)
        valid = slot_valid(counts, MAXRESP)
        context, pull = jax.vjp(lambda a, b, c: attend(a, b, c, counts), query, keys, values)
        summed = inputs.astype(jnp.float32)
        for piece in range(N_TP):
            part = jnp.dot(context[:, piece * head_cols:(piece + 1) * head_cols], w_out[piece * head_cols:(piece + 1) * head_cols], preferred_element_type=jnp.float32)
            summed = summed + rounded(part)
        layer = summed.astype(jnp.bfloat16)
        token_weight = jnp.repeat(weight_row, MAXRESP) * valid.astype(jnp.float32)
        upstream = (token_weight[:, None] * upstream_raw.astype(jnp.float32)).astype(jnp.bfloat16)
        d_context = lax.dot_general(upstream, w_out, (((1,), (1,)), ((), ())), preferred_element_type=jnp.float32).astype(jnp.bfloat16)
        d_parts = pull(d_context)
        sums = []
        for total, grad_in in zip(carry, d_parts):
            term = lax.dot_general(normed, grad_in, (((0,), (0,)), ((), ())), preferred_element_type=jnp.float32)
            sums.append(total + rounded(term))
        return (tuple(sums), layer.reshape(R_DEV, MAXRESP, D))
    start = (jnp.zeros((D, HEADS * HEAD_DIM), jnp.float32), jnp.zeros((D, KV_HEADS * HEAD_DIM), jnp.float32), jnp.zeros((D, KV_HEADS * HEAD_DIM), jnp.float32))
    grads, layers = lax.scan(shard_step, start, jnp.arange(ROWS // R_DEV, dtype=jnp.int32))
    layer_out = layers.reshape(ROWS, MAXRESP, D)
    return (state, advantage, layer_out, grads[0], grads[1], grads[2])
```

```python
import jax
import jax.numpy as jnp
from jax import lax
from jax.experimental import pallas as pl
from jax.experimental.pallas import tpu as pltpu
from jax.sharding import PartitionSpec as P

HEAD_DIM = 128
STEPS = 2
MESH = pl.DeviceIdType.MESH


def norm_rows(values, gain):
    wide = values.astype(jnp.float32)
    meansq = jnp.mean(wide * wide, axis=-1, keepdims=True)
    return (wide * lax.rsqrt(meansq + 1e-06) * gain).astype(jnp.bfloat16)


def rounded(values):
    return lax.optimization_barrier(values.astype(jnp.bfloat16)).astype(jnp.float32)


def decode_attend(query, cache_k, cache_v, lengths, new_k, new_v):
    rows_n = query.shape[0]
    slots = cache_k.shape[1]
    kv_n = cache_k.shape[2] // HEAD_DIM
    per_kv = query.shape[1] // cache_k.shape[2]
    scale = 1.0 / HEAD_DIM**0.5
    quer = query.reshape(rows_n, kv_n, per_kv, HEAD_DIM)
    keys_c = cache_k.reshape(rows_n, slots, kv_n, HEAD_DIM)
    vals_c = cache_v.reshape(rows_n, slots, kv_n, HEAD_DIM)
    keys_n = new_k.reshape(rows_n, -1, kv_n, HEAD_DIM)
    vals_n = new_v.reshape(rows_n, -1, kv_n, HEAD_DIM)
    score_c = (
        jnp.einsum("rkgd,rckd->rkgc", quer, keys_c, preferred_element_type=jnp.float32) * scale
    )
    score_n = (
        jnp.einsum("rkgd,rnkd->rkgn", quer, keys_n, preferred_element_type=jnp.float32) * scale
    )
    live = (jnp.arange(slots, dtype=jnp.int32)[None, :] < lengths[:, None])[:, None, None, :]
    score_c = jnp.where(live, score_c, -1e30)
    scores = jnp.concatenate([score_c, score_n], axis=-1)
    expo = jnp.exp(scores)
    weights = (expo / jnp.sum(expo, axis=-1, keepdims=True)).astype(jnp.bfloat16)
    context = jnp.einsum(
        "rkgc,rckd->rkgd", weights[..., :slots], vals_c, preferred_element_type=jnp.float32
    )
    context = context + jnp.einsum(
        "rkgn,rnkd->rkgd", weights[..., slots:], vals_n, preferred_element_type=jnp.float32
    )
    return context.reshape(rows_n, -1).astype(jnp.bfloat16)


def attend(query, keys, values, counts):
    rows_n = counts.shape[0]
    tokens = query.shape[0]
    length = tokens // rows_n
    kv_n = keys.shape[1] // HEAD_DIM
    per_kv = query.shape[1] // keys.shape[1]
    scale = 1.0 / HEAD_DIM**0.5
    quer = query.reshape(rows_n, length, kv_n, per_kv, HEAD_DIM).astype(jnp.float32)
    keyf = keys.reshape(rows_n, length, kv_n, HEAD_DIM).astype(jnp.float32)
    valf = values.reshape(rows_n, length, kv_n, HEAD_DIM).astype(jnp.float32)
    scores = jnp.einsum("rikgd,rjkd->rkgij", quer, keyf) * scale
    slot = jnp.arange(length, dtype=jnp.int32)
    causal = (slot[None, :] <= slot[:, None])[None, :, :]
    inside = slot[None, None, :] < counts[:, None, None]
    mask = (causal & inside)[:, None, None, :, :]
    scores = jnp.where(mask, scores, -1e30)
    expo = jnp.exp(scores)
    weights = (
        (expo / jnp.sum(expo, axis=-1, keepdims=True)).astype(jnp.bfloat16).astype(jnp.float32)
    )
    context = jnp.einsum("rkgij,rjkd->rikgd", weights, valf)
    return context.reshape(tokens, -1).astype(jnp.bfloat16)


def slot_valid(counts, length):
    slot = jnp.arange(length, dtype=jnp.int32)
    return (slot[None, :] < counts[:, None]).reshape(-1)


def exclusive_rank(labels, classes):
    onehot = (labels[:, None] == jnp.arange(classes, dtype=jnp.int32)[None, :]).astype(jnp.int32)
    return jnp.sum((jnp.cumsum(onehot, axis=0) - onehot) * onehot, axis=1)


def exchange(axis, ident, gathers=(), swaps=()):
    members = lax.axis_size(axis)
    items = tuple(gathers) + tuple(swaps)
    total = len(items)

    def kernel(*refs):
        ins, outs = refs[:total], refs[total : 2 * total]
        send_sem, recv_sem, own_sem = refs[2 * total :]
        me = lax.axis_index(axis)
        peers = [lax.rem(me + off, members) for off in range(1, members)]
        barrier = pltpu.get_barrier_semaphore()
        for peer in peers:
            pl.semaphore_signal(
                barrier, inc=1, device_id={axis: peer}, device_id_type=pl.DeviceIdType.MESH
            )
        pl.semaphore_wait(barrier, members - 1)
        copies = []
        for at, peer in enumerate(peers):
            for which in range(total):
                source = ins[which] if which < len(gathers) else ins[which].at[peer]
                copy = pltpu.make_async_remote_copy(
                    src_ref=source,
                    dst_ref=outs[which].at[me],
                    send_sem=send_sem.at[which * (members - 1) + at],
                    recv_sem=recv_sem.at[which * (members - 1) + at],
                    device_id={axis: peer},
                    device_id_type=pl.DeviceIdType.MESH,
                )
                copy.start()
                copies.append(copy)
        for which in range(total):
            source = ins[which] if which < len(gathers) else ins[which].at[me]
            copy = pltpu.make_async_copy(source, outs[which].at[me], own_sem.at[which])
            copy.start()
            copies.append(copy)
        for copy in copies:
            copy.wait()

    shapes = [(members,) + item.shape for item in gathers] + [item.shape for item in swaps]
    sent = sum(
        2 * item.size * (members if at < len(gathers) else 1) for at, item in enumerate(items)
    )
    return pl.pallas_call(
        kernel,
        out_shape=[jax.ShapeDtypeStruct(sh, item.dtype) for sh, item in zip(shapes, items)],
        in_specs=[pl.BlockSpec(memory_space=pltpu.VMEM)] * total,
        out_specs=[pl.BlockSpec(memory_space=pltpu.VMEM)] * total,
        scratch_shapes=[
            pltpu.SemaphoreType.DMA((total * (members - 1),)),
            pltpu.SemaphoreType.DMA((total * (members - 1),)),
            pltpu.SemaphoreType.DMA((total,)),
        ],
        compiler_params=pltpu.CompilerParams(collective_id=ident, has_side_effects=True),
        cost_estimate=pl.CostEstimate(
            flops=sent * 1000, bytes_accessed=2 * sent, transcendentals=0
        ),
        name=f"exchange_{ident}",
    )(*items)


def side_by_side(parts):
    return jnp.moveaxis(parts, 0, 1).reshape(parts.shape[1], -1)


def cut(values, members):
    return jnp.moveaxis(values.reshape(values.shape[0], members, -1), 1, 0)


def project(rows, weights):
    return jnp.concatenate(
        [jnp.dot(rows, weight, preferred_element_type=jnp.float32) for weight in weights], axis=1
    )


def split_qkv(joined, weights):
    first = weights[0].shape[1]
    second = first + weights[1].shape[1]
    return joined[:, :first], joined[:, first:second], joined[:, second:]


def decode_all(hidden, gain, weights, w_out, cache_keys, cache_values, lengths, reward_vec):
    shards, feats = lax.axis_size("dp"), lax.axis_size("tp")
    rows, dim = hidden.shape
    slots = cache_keys.shape[1]
    wide = dim // feats
    per = feats // shards
    heads = weights[0].shape[1] // HEAD_DIM
    join = sum(w.shape[1] for w in weights)
    qcols = weights[0].shape[1]
    scale = 1.0 / HEAD_DIM**0.5
    tall = heads * rows
    extra = HEAD_DIM
    dims = (((1,), (1,)), ((), ()))

    def kernel(
        hid, gain_r, len_r, rvec, ck_h, cv_h, wq_h, wk_h, wv_h, wo_h,
        dec_o, adv_o,
        wq, wk, wv, wo, ck, cv,
        st, nsend, nbuf, psend, pbuf, osend, obuf, snew, kn, vn, rbuf,
        lsem, hs, hr, ps, pr, os_, or_, ss, sr, rs, rr,
    ):
        me_d, me_t = lax.axis_index("dp"), lax.axis_index("tp")
        loads = []
        for at, (src, dst) in enumerate(
            ((wq_h, wq), (wk_h, wk), (wv_h, wv), (ck_h, ck), (cv_h, cv), (wo_h, wo))
        ):
            loads.append(pltpu.make_async_copy(src, dst, lsem.at[at]))
            loads[-1].start()
        barrier = pltpu.get_barrier_semaphore()
        for off in range(1, shards):
            pl.semaphore_signal(
                barrier, inc=1, device_id={"dp": lax.rem(me_d + off, shards)}, device_id_type=MESH
            )
        for off in range(1, feats):
            pl.semaphore_signal(
                barrier, inc=1, device_id={"tp": lax.rem(me_t + off, feats)}, device_id_type=MESH
            )
        for q in range(feats):
            st[q] = hid[:, q * wide : (q + 1) * wide]
        kn[...] = jnp.zeros_like(kn)
        vn[...] = jnp.zeros_like(vn)
        lens = jnp.concatenate([len_r[...]] * heads, axis=0)
        row_c = lax.broadcasted_iota(jnp.int32, (tall, rows * slots), 0) % rows
        col_c = lax.broadcasted_iota(jnp.int32, (tall, rows * slots), 1)
        live_c = (col_c // slots == row_c) & (col_c % slots < lens)
        row_n = lax.broadcasted_iota(jnp.int32, (tall, extra), 0) % rows
        col_n = lax.broadcasted_iota(jnp.int32, (tall, extra), 1)
        pl.semaphore_wait(barrier, shards - 1 + feats - 1)

        for step in range(STEPS):
            total = jnp.zeros((rows, 1), jnp.float32)
            for q in range(feats):
                cell = st[q].astype(jnp.float32)
                total = total + jnp.sum(cell * cell, axis=1, keepdims=True)
            inv = lax.rsqrt(total / dim + 1e-06)
            for q in range(feats):
                nsend[step, q] = (
                    st[q].astype(jnp.float32) * inv * gain_r[:, q * wide : (q + 1) * wide]
                ).astype(jnp.bfloat16)
            copies = []
            for off in range(1, shards):
                peer = lax.rem(me_d + off, shards)
                copies.append(
                    pltpu.make_async_remote_copy(
                        src_ref=nsend.at[step, pl.ds(peer * per, per)],
                        dst_ref=nbuf.at[step, me_d],
                        send_sem=hs.at[step, off - 1],
                        recv_sem=hr.at[step, off - 1],
                        device_id={"dp": peer},
                        device_id_type=MESH,
                    )
                )
                copies[-1].start()
            nbuf[step, me_d] = nsend[step, pl.ds(me_d * per, per)]
            if step == 0:
                for one in loads[:3]:
                    one.wait()
            for copy in copies:
                copy.wait()
            parts = []
            for w in (wq, wk, wv):
                acc = None
                for q in range(per):
                    left = jnp.concatenate([nbuf[step, s, q] for s in range(shards)], axis=0)
                    one = jnp.dot(
                        left, w[q * wide : (q + 1) * wide], preferred_element_type=jnp.float32
                    )
                    acc = one if acc is None else acc + one
                parts.append(acc)
            part = jnp.concatenate(parts, axis=1)
            for s in range(shards):
                psend[step, s] = part[s * rows : (s + 1) * rows]
            copies = []
            for off in range(1, shards):
                peer = lax.rem(me_d + off, shards)
                copies.append(
                    pltpu.make_async_remote_copy(
                        src_ref=psend.at[step, peer],
                        dst_ref=pbuf.at[step, me_d],
                        send_sem=ps.at[step, off - 1],
                        recv_sem=pr.at[step, off - 1],
                        device_id={"dp": peer},
                        device_id_type=MESH,
                    )
                )
                copies[-1].start()
            pbuf[step, me_d] = psend[step, me_d]
            if step == 0:
                for one in loads[3:]:
                    one.wait()
            for copy in copies:
                copy.wait()
            joined = pbuf[step, 0]
            for s in range(1, shards):
                joined = joined + pbuf[step, s]
            joined = joined.astype(jnp.bfloat16)
            query = jnp.concatenate(
                [joined[:, h * HEAD_DIM : (h + 1) * HEAD_DIM] for h in range(heads)], axis=0
            )
            kn[step * rows : (step + 1) * rows] = joined[:, qcols : qcols + HEAD_DIM]
            vn[step * rows : (step + 1) * rows] = joined[:, qcols + HEAD_DIM :]
            score_c = (
                lax.dot_general(query, ck[...], dims, preferred_element_type=jnp.float32) * scale
            )
            score_n = (
                lax.dot_general(query, kn[...], dims, preferred_element_type=jnp.float32) * scale
            )
            expo_c = jnp.where(live_c, jnp.exp(jnp.where(live_c, score_c, 0.0)), 0.0)
            live_n = (col_n % rows == row_n) & (col_n < (step + 1) * rows)
            expo_n = jnp.where(live_n, jnp.exp(jnp.where(live_n, score_n, 0.0)), 0.0)
            denom = jnp.sum(expo_c, axis=1, keepdims=True) + jnp.sum(expo_n, axis=1, keepdims=True)
            soft_c = (expo_c / denom).astype(jnp.bfloat16)
            soft_n = (expo_n / denom).astype(jnp.bfloat16)
            ctx = (
                jnp.dot(soft_c, cv[...], preferred_element_type=jnp.float32)
                + jnp.dot(soft_n, vn[...], preferred_element_type=jnp.float32)
            ).astype(jnp.bfloat16)
            context = jnp.concatenate(
                [ctx[h * rows : (h + 1) * rows] for h in range(heads)], axis=1
            )
            for q in range(feats):
                osend[step, q] = jnp.dot(
                    context, wo[:, q * wide : (q + 1) * wide], preferred_element_type=jnp.float32
                ).astype(jnp.bfloat16)
            copies = []
            for off in range(1, feats):
                peer = lax.rem(me_t + off, feats)
                copies.append(
                    pltpu.make_async_remote_copy(
                        src_ref=osend.at[step, peer],
                        dst_ref=obuf.at[step, me_t],
                        send_sem=os_.at[step, off - 1],
                        recv_sem=or_.at[step, off - 1],
                        device_id={"tp": peer},
                        device_id_type=MESH,
                    )
                )
                copies[-1].start()
            obuf[step, me_t] = osend[step, me_t]
            for copy in copies:
                copy.wait()
            acc = st[me_t].astype(jnp.float32)
            for s in range(feats):
                acc = acc + obuf[step, s].astype(jnp.float32)
            snew[step, me_t] = acc.astype(jnp.bfloat16)
            copies = []
            for off in range(1, feats):
                peer = lax.rem(me_t + off, feats)
                copies.append(
                    pltpu.make_async_remote_copy(
                        src_ref=snew.at[step, me_t],
                        dst_ref=snew.at[step, me_t],
                        send_sem=ss.at[step, off - 1],
                        recv_sem=sr.at[step, off - 1],
                        device_id={"tp": peer},
                        device_id_type=MESH,
                    )
                )
                copies[-1].start()
            for copy in copies:
                copy.wait()
            for q in range(feats):
                st[q] = snew[step, q]

        reward = jnp.zeros((rows, 1), jnp.float32)
        for q in range(feats):
            dec_o[:, q * wide : (q + 1) * wide] = st[q]
            reward = reward + jnp.sum(
                st[q].astype(jnp.float32) * rvec[:, q * wide : (q + 1) * wide],
                axis=1,
                keepdims=True,
            )
        rbuf[me_d] = jnp.broadcast_to(reward, (rows, HEAD_DIM))
        copies = []
        for off in range(1, shards):
            peer = lax.rem(me_d + off, shards)
            copies.append(
                pltpu.make_async_remote_copy(
                    src_ref=rbuf.at[me_d],
                    dst_ref=rbuf.at[me_d],
                    send_sem=rs.at[off - 1],
                    recv_sem=rr.at[off - 1],
                    device_id={"dp": peer},
                    device_id_type=MESH,
                )
            )
            copies[-1].start()
        for copy in copies:
            copy.wait()
        count = shards * rows
        every = jnp.concatenate([rbuf[s] for s in range(shards)], axis=0)
        mean = jnp.sum(every, axis=0, keepdims=True) / count
        spread = jnp.sum(every * every, axis=0, keepdims=True) / count - mean * mean
        adv_o[...] = (every - mean) / jnp.sqrt(spread + 1e-05)

    bf, f32 = jnp.bfloat16, jnp.float32
    dma = pltpu.SemaphoreType.DMA
    vmem, hbm = pl.BlockSpec(memory_space=pltpu.VMEM), pl.BlockSpec(memory_space=pl.ANY)
    flops = 2 * STEPS * dim * (join + qcols) * rows * 2
    return pl.pallas_call(
        kernel,
        out_shape=[
            jax.ShapeDtypeStruct((rows, dim), bf),
            jax.ShapeDtypeStruct((shards * rows, HEAD_DIM), f32),
        ],
        in_specs=[vmem] * 4 + [hbm] * 6,
        out_specs=[vmem] * 2,
        scratch_shapes=[
            pltpu.VMEM(weights[0].shape, bf),
            pltpu.VMEM(weights[1].shape, bf),
            pltpu.VMEM(weights[2].shape, bf),
            pltpu.VMEM(w_out.shape, bf),
            pltpu.VMEM((rows * slots, HEAD_DIM), bf),
            pltpu.VMEM((rows * slots, HEAD_DIM), bf),
            pltpu.VMEM((feats, rows, wide), bf),
            pltpu.VMEM((STEPS, feats, rows, wide), bf),
            pltpu.VMEM((STEPS, shards, per, rows, wide), bf),
            pltpu.VMEM((STEPS, shards, rows, join), f32),
            pltpu.VMEM((STEPS, shards, rows, join), f32),
            pltpu.VMEM((STEPS, feats, rows, wide), bf),
            pltpu.VMEM((STEPS, feats, rows, wide), bf),
            pltpu.VMEM((STEPS, feats, rows, wide), bf),
            pltpu.VMEM((extra, HEAD_DIM), bf),
            pltpu.VMEM((extra, HEAD_DIM), bf),
            pltpu.VMEM((shards, rows, HEAD_DIM), f32),
            dma((6,)),
            dma((STEPS, shards - 1)),
            dma((STEPS, shards - 1)),
            dma((STEPS, shards - 1)),
            dma((STEPS, shards - 1)),
            dma((STEPS, feats - 1)),
            dma((STEPS, feats - 1)),
            dma((STEPS, feats - 1)),
            dma((STEPS, feats - 1)),
            dma((shards - 1,)),
            dma((shards - 1,)),
        ],
        compiler_params=pltpu.CompilerParams(collective_id=4, has_side_effects=True),
        cost_estimate=pl.CostEstimate(
            flops=40_000_000_000, bytes_accessed=2 * (join + qcols) * dim, transcendentals=0
        ),
        name="decode_all",
    )(
        hidden,
        gain.reshape(1, -1),
        lengths.reshape(-1, 1),
        reward_vec.reshape(1, -1),
        cache_keys.reshape(rows * slots, -1),
        cache_values.reshape(rows * slots, -1),
        *weights,
        w_out,
    )


def on_device_plain(
    hidden_last,
    gain,
    w_query,
    w_key,
    w_value,
    w_out,
    cache_keys,
    cache_values,
    cache_lengths,
    reward_vec,
    response_counts,
    assignment,
    responses,
    cotangent,
):
    shards = lax.axis_size("dp")
    feats = lax.axis_size("tp")
    myself = lax.axis_index("dp")
    weights = (w_query, w_key, w_value)
    rows_dev, length, _ = responses.shape
    tokens = rows_dev * length
    group_rows = assignment.shape[0]

    positions = jnp.arange(group_rows, dtype=jnp.int32)
    place = assignment * rows_dev + exclusive_rank(assignment, shards)
    order = jnp.sum(jnp.where(place[None, :] == positions[:, None], positions[None, :], 0), axis=1)
    chosen = lax.dynamic_slice_in_dim(order, myself * rows_dev, rows_dev)

    (row_parts,) = exchange("tp", 0, gathers=(responses.reshape(tokens, -1),))
    own_normed = norm_rows(side_by_side(row_parts), gain)
    (block,) = exchange("dp", 1, swaps=(cut(own_normed, shards),))
    width = block.shape[-1]
    block = jnp.take(block.reshape(group_rows, length, width), order, axis=0)
    block = block.reshape(group_rows * length, width)
    share = group_rows * length // feats
    every_block = lax.all_gather(
        lax.dynamic_slice_in_dim(block, lax.axis_index("tp") * share, share),
        ("grp", "tp"),
        axis=0,
        tiled=True,
    )

    joined = project(block, weights).astype(jnp.bfloat16)
    mine_x = jnp.take(
        lax.all_gather(responses, "dp", axis=0, tiled=True), chosen, axis=0
    ).reshape(tokens, -1)
    (joined_parts,) = exchange("dp", 2, swaps=(joined.reshape(shards, tokens, -1),))
    joined = jnp.sum(joined_parts.astype(jnp.float32), axis=0).astype(jnp.bfloat16)
    query, keys, values = split_qkv(joined, weights)
    counts = jnp.take(response_counts, chosen)
    valid = slot_valid(counts, length)
    context, pull = jax.vjp(lambda a, b, c: attend(a, b, c, counts), query, keys, values)
    partial_out = jnp.dot(context, w_out, preferred_element_type=jnp.float32)
    layer = (
        mine_x.astype(jnp.float32)
        + lax.psum_scatter(
            partial_out.astype(jnp.bfloat16), "tp", scatter_dimension=1, tiled=True
        ).astype(jnp.float32)
    ).astype(jnp.bfloat16)

    local_cot = cotangent.reshape(tokens, -1) * valid.astype(jnp.bfloat16)[:, None]
    (cot_parts,) = exchange("tp", 3, gathers=(local_cot,))
    d_context = lax.dot_general(
        side_by_side(cot_parts),
        w_out,
        (((1,), (1,)), ((), ())),
        preferred_element_type=jnp.float32,
    ).astype(jnp.bfloat16)
    d_joined = jnp.concatenate(pull(d_context), axis=1)

    state = hidden_last
    keys_new = []
    values_new = []
    for step in range(STEPS):
        normed = norm_rows(state, gain)
        (pieces,) = exchange("dp", 4 + 3 * step, swaps=(cut(normed, shards),))
        part = project(pieces.reshape(group_rows, -1), weights)
        (parts,) = exchange("dp", 5 + 3 * step, swaps=(part.reshape(shards, rows_dev, -1),))
        step_q, step_k, step_v = split_qkv(
            jnp.sum(parts, axis=0).astype(jnp.bfloat16), weights
        )
        keys_new.append(step_k)
        values_new.append(step_v)
        step_context = decode_attend(
            step_q,
            cache_keys,
            cache_values,
            cache_lengths,
            jnp.stack(keys_new, 1),
            jnp.stack(values_new, 1),
        )
        step_out = jnp.dot(step_context, w_out, preferred_element_type=jnp.float32)
        (outs,) = exchange("tp", 6 + 3 * step, gathers=(step_out.astype(jnp.bfloat16),))
        state = (
            state.astype(jnp.float32) + jnp.sum(outs.astype(jnp.float32), axis=0)
        ).astype(jnp.bfloat16)
    reward = jnp.sum(state.astype(jnp.float32) * reward_vec, axis=-1, keepdims=True)
    (every_reward,) = exchange(
        "dp", 4 + 3 * STEPS, gathers=(jnp.broadcast_to(reward, (rows_dev, HEAD_DIM)),)
    )
    rewards = every_reward[:, :, 0].reshape(-1)
    mean = jnp.sum(rewards) / group_rows
    spread = jnp.sum(rewards * rewards) / group_rows - mean * mean
    every_adv = (rewards - mean) / jnp.sqrt(spread + 1e-05)
    advantage = lax.dynamic_slice_in_dim(every_adv, myself * rows_dev, rows_dev)
    my_adv = jnp.take(every_adv.astype(jnp.bfloat16), chosen).astype(jnp.float32)

    scaled = (jnp.repeat(my_adv, length)[:, None] * d_joined.astype(jnp.float32)).astype(
        jnp.bfloat16
    )
    every_d = lax.all_gather(scaled, ("grp", "dp"), axis=0, tiled=True)
    grad_q, grad_k, grad_v = (
        lax.dot_general(
            every_block, piece, (((0,), (0,)), ((), ())), preferred_element_type=jnp.float32
        )
        for piece in split_qkv(every_d, weights)
    )
    return (state, advantage, layer.reshape(rows_dev, length, -1), grad_q, grad_k, grad_v)


def on_device(
    hidden_last,
    gain,
    w_query,
    w_key,
    w_value,
    w_out,
    cache_keys,
    cache_values,
    cache_lengths,
    reward_vec,
    response_counts,
    assignment,
    responses,
    cotangent,
):
    shards = lax.axis_size("dp")
    feats = lax.axis_size("tp")
    myself = lax.axis_index("dp")
    weights = (w_query, w_key, w_value)
    rows_dev, length, _ = responses.shape
    tokens = rows_dev * length
    group_rows = assignment.shape[0]

    positions = jnp.arange(group_rows, dtype=jnp.int32)
    place = assignment * rows_dev + exclusive_rank(assignment, shards)
    order = jnp.sum(jnp.where(place[None, :] == positions[:, None], positions[None, :], 0), axis=1)
    chosen = lax.dynamic_slice_in_dim(order, myself * rows_dev, rows_dev)

    (row_parts,) = exchange("tp", 0, gathers=(responses.reshape(tokens, -1),))
    own_normed = norm_rows(side_by_side(row_parts), gain)
    (block,) = exchange("dp", 1, swaps=(cut(own_normed, shards),))
    width = block.shape[-1]
    block = jnp.take(block.reshape(group_rows, length, width), order, axis=0)
    block = block.reshape(group_rows * length, width)
    share = group_rows * length // feats
    every_block = lax.all_gather(
        lax.dynamic_slice_in_dim(block, lax.axis_index("tp") * share, share),
        ("grp", "tp"),
        axis=0,
        tiled=True,
    )

    joined = project(block, weights).astype(jnp.bfloat16)
    mine_x = jnp.take(
        lax.all_gather(responses, "dp", axis=0, tiled=True), chosen, axis=0
    ).reshape(tokens, -1)
    (joined_parts,) = exchange("dp", 2, swaps=(joined.reshape(shards, tokens, -1),))
    joined = jnp.sum(joined_parts.astype(jnp.float32), axis=0).astype(jnp.bfloat16)
    query, keys, values = split_qkv(joined, weights)
    counts = jnp.take(response_counts, chosen)
    valid = slot_valid(counts, length)
    context, pull = jax.vjp(lambda a, b, c: attend(a, b, c, counts), query, keys, values)
    partial_out = jnp.dot(context, w_out, preferred_element_type=jnp.float32)
    layer = (
        mine_x.astype(jnp.float32)
        + lax.psum_scatter(
            partial_out.astype(jnp.bfloat16), "tp", scatter_dimension=1, tiled=True
        ).astype(jnp.float32)
    ).astype(jnp.bfloat16)

    local_cot = cotangent.reshape(tokens, -1) * valid.astype(jnp.bfloat16)[:, None]
    (cot_parts,) = exchange("tp", 3, gathers=(local_cot,))
    d_context = lax.dot_general(
        side_by_side(cot_parts),
        w_out,
        (((1,), (1,)), ((), ())),
        preferred_element_type=jnp.float32,
    ).astype(jnp.bfloat16)
    d_joined = jnp.concatenate(pull(d_context), axis=1)

    every_d = lax.all_gather(d_joined, ("grp", "dp"), axis=0, tiled=True)

    state, every_adv = decode_all(
        hidden_last, gain, weights, w_out, cache_keys, cache_values, cache_lengths, reward_vec
    )
    every_adv = every_adv[:, 0]
    advantage = lax.dynamic_slice_in_dim(every_adv, myself * rows_dev, rows_dev)
    group_adv = jnp.take(every_adv.astype(jnp.bfloat16), order).astype(jnp.float32)
    (all_adv,) = exchange(
        "grp", 5, gathers=(jnp.broadcast_to(group_adv[:, None], (group_rows, HEAD_DIM)),)
    )
    token_adv = jnp.repeat(all_adv[:, :, 0].reshape(-1), length)
    every_d = (token_adv[:, None] * every_d.astype(jnp.float32)).astype(jnp.bfloat16)
    grad_q, grad_k, grad_v = (
        lax.dot_general(
            every_block, piece, (((0,), (0,)), ((), ())), preferred_element_type=jnp.float32
        )
        for piece in split_qkv(every_d, weights)
    )
    return (state, advantage, layer.reshape(rows_dev, length, -1), grad_q, grad_k, grad_v)


def solution(mesh):
    whole_halves = mesh.shape["tp"] % mesh.shape["dp"] == 0
    return jax.shard_map(
        on_device if whole_halves else on_device_plain,
        mesh=mesh,
        in_specs=(
            P(("grp", "dp"), None),
            P(),
            P("dp", "tp"),
            P("dp", "tp"),
            P("dp", "tp"),
            P("tp", None),
            P(("grp", "dp"), None, "tp"),
            P(("grp", "dp"), None, "tp"),
            P(("grp", "dp")),
            P(),
            P("grp"),
            P("grp"),
            P(("grp", "dp"), None, "tp"),
            P(("grp", "dp"), None, "tp"),
        ),
        out_specs=(
            P(("grp", "dp"), None),
            P(("grp", "dp")),
            P(("grp", "dp"), None, "tp"),
            P("dp", "tp"),
            P("dp", "tp"),
            P("dp", "tp"),
        ),
        check_vma=False,
    )
```

```python
import jax
import jax.numpy as jnp
from jax import lax
from jax.experimental import pallas as pl
from jax.experimental.pallas import tpu as pltpu
from jax.sharding import PartitionSpec as P

HEAD_DIM = 128
STEPS = 2
MESH = pl.DeviceIdType.MESH


def norm_rows(values, gain):
    wide = values.astype(jnp.float32)
    meansq = jnp.mean(wide * wide, axis=-1, keepdims=True)
    return (wide * lax.rsqrt(meansq + 1e-06) * gain).astype(jnp.bfloat16)


def rounded(values):
    return lax.optimization_barrier(values.astype(jnp.bfloat16)).astype(jnp.float32)


def decode_attend(query, cache_k, cache_v, lengths, new_k, new_v):
    rows_n = query.shape[0]
    slots = cache_k.shape[1]
    kv_n = cache_k.shape[2] // HEAD_DIM
    per_kv = query.shape[1] // cache_k.shape[2]
    scale = 1.0 / HEAD_DIM**0.5
    quer = query.reshape(rows_n, kv_n, per_kv, HEAD_DIM)
    keys_c = cache_k.reshape(rows_n, slots, kv_n, HEAD_DIM)
    vals_c = cache_v.reshape(rows_n, slots, kv_n, HEAD_DIM)
    keys_n = new_k.reshape(rows_n, -1, kv_n, HEAD_DIM)
    vals_n = new_v.reshape(rows_n, -1, kv_n, HEAD_DIM)
    score_c = (
        jnp.einsum("rkgd,rckd->rkgc", quer, keys_c, preferred_element_type=jnp.float32) * scale
    )
    score_n = (
        jnp.einsum("rkgd,rnkd->rkgn", quer, keys_n, preferred_element_type=jnp.float32) * scale
    )
    live = (jnp.arange(slots, dtype=jnp.int32)[None, :] < lengths[:, None])[:, None, None, :]
    score_c = jnp.where(live, score_c, -1e30)
    scores = jnp.concatenate([score_c, score_n], axis=-1)
    expo = jnp.exp(scores)
    weights = (expo / jnp.sum(expo, axis=-1, keepdims=True)).astype(jnp.bfloat16)
    context = jnp.einsum(
        "rkgc,rckd->rkgd", weights[..., :slots], vals_c, preferred_element_type=jnp.float32
    )
    context = context + jnp.einsum(
        "rkgn,rnkd->rkgd", weights[..., slots:], vals_n, preferred_element_type=jnp.float32
    )
    return context.reshape(rows_n, -1).astype(jnp.bfloat16)


def attend(query, keys, values, counts):
    rows_n = counts.shape[0]
    tokens = query.shape[0]
    length = tokens // rows_n
    kv_n = keys.shape[1] // HEAD_DIM
    per_kv = query.shape[1] // keys.shape[1]
    scale = 1.0 / HEAD_DIM**0.5
    quer = query.reshape(rows_n, length, kv_n, per_kv, HEAD_DIM).astype(jnp.float32)
    keyf = keys.reshape(rows_n, length, kv_n, HEAD_DIM).astype(jnp.float32)
    valf = values.reshape(rows_n, length, kv_n, HEAD_DIM).astype(jnp.float32)
    scores = jnp.einsum("rikgd,rjkd->rkgij", quer, keyf) * scale
    slot = jnp.arange(length, dtype=jnp.int32)
    causal = (slot[None, :] <= slot[:, None])[None, :, :]
    inside = slot[None, None, :] < counts[:, None, None]
    mask = (causal & inside)[:, None, None, :, :]
    scores = jnp.where(mask, scores, -1e30)
    expo = jnp.exp(scores)
    weights = (
        (expo / jnp.sum(expo, axis=-1, keepdims=True)).astype(jnp.bfloat16).astype(jnp.float32)
    )
    context = jnp.einsum("rkgij,rjkd->rikgd", weights, valf)
    return context.reshape(tokens, -1).astype(jnp.bfloat16)


def slot_valid(counts, length):
    slot = jnp.arange(length, dtype=jnp.int32)
    return (slot[None, :] < counts[:, None]).reshape(-1)


def exclusive_rank(labels, classes):
    onehot = (labels[:, None] == jnp.arange(classes, dtype=jnp.int32)[None, :]).astype(jnp.int32)
    return jnp.sum((jnp.cumsum(onehot, axis=0) - onehot) * onehot, axis=1)


def exchange(axis, ident, gathers=(), swaps=()):
    members = lax.axis_size(axis)
    items = tuple(gathers) + tuple(swaps)
    total = len(items)

    def kernel(*refs):
        ins, outs = refs[:total], refs[total : 2 * total]
        send_sem, recv_sem, own_sem = refs[2 * total :]
        me = lax.axis_index(axis)
        peers = [lax.rem(me + off, members) for off in range(1, members)]
        barrier = pltpu.get_barrier_semaphore()
        for peer in peers:
            pl.semaphore_signal(
                barrier, inc=1, device_id={axis: peer}, device_id_type=pl.DeviceIdType.MESH
            )
        pl.semaphore_wait(barrier, members - 1)
        copies = []
        for at, peer in enumerate(peers):
            for which in range(total):
                source = ins[which] if which < len(gathers) else ins[which].at[peer]
                copy = pltpu.make_async_remote_copy(
                    src_ref=source,
                    dst_ref=outs[which].at[me],
                    send_sem=send_sem.at[which * (members - 1) + at],
                    recv_sem=recv_sem.at[which * (members - 1) + at],
                    device_id={axis: peer},
                    device_id_type=pl.DeviceIdType.MESH,
                )
                copy.start()
                copies.append(copy)
        for which in range(total):
            source = ins[which] if which < len(gathers) else ins[which].at[me]
            copy = pltpu.make_async_copy(source, outs[which].at[me], own_sem.at[which])
            copy.start()
            copies.append(copy)
        for copy in copies:
            copy.wait()

    shapes = [(members,) + item.shape for item in gathers] + [item.shape for item in swaps]
    sent = sum(
        2 * item.size * (members if at < len(gathers) else 1) for at, item in enumerate(items)
    )
    return pl.pallas_call(
        kernel,
        out_shape=[jax.ShapeDtypeStruct(sh, item.dtype) for sh, item in zip(shapes, items)],
        in_specs=[pl.BlockSpec(memory_space=pltpu.VMEM)] * total,
        out_specs=[pl.BlockSpec(memory_space=pltpu.VMEM)] * total,
        scratch_shapes=[
            pltpu.SemaphoreType.DMA((total * (members - 1),)),
            pltpu.SemaphoreType.DMA((total * (members - 1),)),
            pltpu.SemaphoreType.DMA((total,)),
        ],
        compiler_params=pltpu.CompilerParams(collective_id=ident, has_side_effects=True),
        cost_estimate=pl.CostEstimate(
            flops=sent * 1000, bytes_accessed=2 * sent, transcendentals=0
        ),
        name=f"exchange_{ident}",
    )(*items)


def side_by_side(parts):
    return jnp.moveaxis(parts, 0, 1).reshape(parts.shape[1], -1)


def cut(values, members):
    return jnp.moveaxis(values.reshape(values.shape[0], members, -1), 1, 0)


def project(rows, weights):
    return jnp.concatenate(
        [jnp.dot(rows, weight, preferred_element_type=jnp.float32) for weight in weights], axis=1
    )


def split_qkv(joined, weights):
    first = weights[0].shape[1]
    second = first + weights[1].shape[1]
    return joined[:, :first], joined[:, first:second], joined[:, second:]


def on_device_plain(
    hidden_last,
    gain,
    w_query,
    w_key,
    w_value,
    w_out,
    cache_keys,
    cache_values,
    cache_lengths,
    reward_vec,
    response_counts,
    assignment,
    responses,
    cotangent,
):
    shards = lax.axis_size("dp")
    feats = lax.axis_size("tp")
    myself = lax.axis_index("dp")
    weights = (w_query, w_key, w_value)
    rows_dev, length, _ = responses.shape
    tokens = rows_dev * length
    group_rows = assignment.shape[0]

    positions = jnp.arange(group_rows, dtype=jnp.int32)
    place = assignment * rows_dev + exclusive_rank(assignment, shards)
    order = jnp.sum(jnp.where(place[None, :] == positions[:, None], positions[None, :], 0), axis=1)
    chosen = lax.dynamic_slice_in_dim(order, myself * rows_dev, rows_dev)

    (row_parts,) = exchange("tp", 0, gathers=(responses.reshape(tokens, -1),))
    own_normed = norm_rows(side_by_side(row_parts), gain)
    (block,) = exchange("dp", 1, swaps=(cut(own_normed, shards),))
    width = block.shape[-1]
    block = jnp.take(block.reshape(group_rows, length, width), order, axis=0)
    block = block.reshape(group_rows * length, width)
    share = group_rows * length // feats
    every_block = lax.all_gather(
        lax.dynamic_slice_in_dim(block, lax.axis_index("tp") * share, share),
        ("grp", "tp"),
        axis=0,
        tiled=True,
    )

    joined = project(block, weights).astype(jnp.bfloat16)
    mine_x = jnp.take(
        lax.all_gather(responses, "dp", axis=0, tiled=True), chosen, axis=0
    ).reshape(tokens, -1)
    (joined_parts,) = exchange("dp", 2, swaps=(joined.reshape(shards, tokens, -1),))
    joined = jnp.sum(joined_parts.astype(jnp.float32), axis=0).astype(jnp.bfloat16)
    query, keys, values = split_qkv(joined, weights)
    counts = jnp.take(response_counts, chosen)
    valid = slot_valid(counts, length)
    context, pull = jax.vjp(lambda a, b, c: attend(a, b, c, counts), query, keys, values)
    partial_out = jnp.dot(context, w_out, preferred_element_type=jnp.float32)
    layer = (
        mine_x.astype(jnp.float32)
        + lax.psum_scatter(
            partial_out.astype(jnp.bfloat16), "tp", scatter_dimension=1, tiled=True
        ).astype(jnp.float32)
    ).astype(jnp.bfloat16)

    local_cot = cotangent.reshape(tokens, -1) * valid.astype(jnp.bfloat16)[:, None]
    (cot_parts,) = exchange("tp", 3, gathers=(local_cot,))
    d_context = lax.dot_general(
        side_by_side(cot_parts),
        w_out,
        (((1,), (1,)), ((), ())),
        preferred_element_type=jnp.float32,
    ).astype(jnp.bfloat16)
    d_joined = jnp.concatenate(pull(d_context), axis=1)

    state = hidden_last
    keys_new = []
    values_new = []
    for step in range(STEPS):
        normed = norm_rows(state, gain)
        (pieces,) = exchange("dp", 4 + 3 * step, swaps=(cut(normed, shards),))
        part = project(pieces.reshape(group_rows, -1), weights)
        (parts,) = exchange("dp", 5 + 3 * step, swaps=(part.reshape(shards, rows_dev, -1),))
        step_q, step_k, step_v = split_qkv(
            jnp.sum(parts, axis=0).astype(jnp.bfloat16), weights
        )
        keys_new.append(step_k)
        values_new.append(step_v)
        step_context = decode_attend(
            step_q,
            cache_keys,
            cache_values,
            cache_lengths,
            jnp.stack(keys_new, 1),
            jnp.stack(values_new, 1),
        )
        step_out = jnp.dot(step_context, w_out, preferred_element_type=jnp.float32)
        (outs,) = exchange("tp", 6 + 3 * step, gathers=(step_out.astype(jnp.bfloat16),))
        state = (
            state.astype(jnp.float32) + jnp.sum(outs.astype(jnp.float32), axis=0)
        ).astype(jnp.bfloat16)
    reward = jnp.sum(state.astype(jnp.float32) * reward_vec, axis=-1, keepdims=True)
    (every_reward,) = exchange(
        "dp", 4 + 3 * STEPS, gathers=(jnp.broadcast_to(reward, (rows_dev, HEAD_DIM)),)
    )
    rewards = every_reward[:, :, 0].reshape(-1)
    mean = jnp.sum(rewards) / group_rows
    spread = jnp.sum(rewards * rewards) / group_rows - mean * mean
    every_adv = (rewards - mean) / jnp.sqrt(spread + 1e-05)
    advantage = lax.dynamic_slice_in_dim(every_adv, myself * rows_dev, rows_dev)
    my_adv = jnp.take(every_adv.astype(jnp.bfloat16), chosen).astype(jnp.float32)

    scaled = (jnp.repeat(my_adv, length)[:, None] * d_joined.astype(jnp.float32)).astype(
        jnp.bfloat16
    )
    every_d = lax.all_gather(scaled, ("grp", "dp"), axis=0, tiled=True)
    grad_q, grad_k, grad_v = (
        lax.dot_general(
            every_block, piece, (((0,), (0,)), ((), ())), preferred_element_type=jnp.float32
        )
        for piece in split_qkv(every_d, weights)
    )
    return (state, advantage, layer.reshape(rows_dev, length, -1), grad_q, grad_k, grad_v)


def front(length, own_x, own_cot, gain, source, counts, weights, w_out):
    shards, feats = lax.axis_size("dp"), lax.axis_size("tp")
    tokens, wide = own_x.shape
    half = weights[0].shape[0]
    every = shards * tokens
    heads = weights[0].shape[1] // HEAD_DIM
    qcols = weights[0].shape[1]
    join = sum(w.shape[1] for w in weights)
    pieces = 4
    size = tokens // pieces
    scale = 1.0 / HEAD_DIM**0.5
    nt = (((1,), (1,)), ((), ()))
    tn = (((0,), (0,)), ((), ()))
    bf, f32 = jnp.bfloat16, jnp.float32

    def kernel(
        x_h, cot_h, gain_r, src_r, cnt_r, wq_h, wk_h, wv_h, wo_h,
        blk_o, d_o, part_o, mine_o,
        wq, wk, wv, wo, both, xbuf, sibd, sibx, mbuf, cotf, sbuf, inv_s, nb, pm,
        jsend, jrecv, qs, dcs, ws, dss,
        lsem, s_s, s_r, y_s, y_r, x_s, x_r, a_s, a_r, b_s, b_r, c_s, c_r, j_s, j_r,
    ):
        me_d, me_t = lax.axis_index("dp"), lax.axis_index("tp")
        other = 1 - me_d
        core = lax.rem(me_t, 2)
        sib = me_t + 1 - 2 * core
        across = lax.rem(me_t + 2, feats)
        relay = lax.rem(me_t // 2 + me_d + 1, 2)
        home = 1 - relay
        load_x = pltpu.make_async_copy(x_h, both.at[0], lsem.at[0])
        load_x.start()
        load_c = pltpu.make_async_copy(cot_h, cotf.at[me_t], lsem.at[1])
        load_c.start()
        loads = []
        for at, (src, dst) in enumerate(((wq_h, wq), (wk_h, wk), (wv_h, wv), (wo_h, wo))):
            loads.append(pltpu.make_async_copy(src, dst, lsem.at[2 + at]))
            loads[-1].start()
        barrier = pltpu.get_barrier_semaphore()
        peers = []
        for off in range(1, shards * feats):
            at = lax.rem(me_d * feats + me_t + off, shards * feats)
            peers.append({"dp": at // feats, "tp": lax.rem(at, feats)})
            pl.semaphore_signal(barrier, inc=1, device_id=peers[-1], device_id_type=MESH)
        pl.semaphore_wait(barrier, shards * feats - 1)
        load_x.wait()
        load_c.wait()

        def remote(src, dst, send, recv, target):
            copy = pltpu.make_async_remote_copy(
                src_ref=src,
                dst_ref=dst,
                send_sem=send,
                recv_sem=recv,
                device_id=target,
                device_id_type=MESH,
            )
            copy.start()
            return copy

        to_x, to_y, to_sib = {"dp": other}, {"tp": across}, {"tp": sib}
        cut_at = [pl.ds(i * size, size) for i in range(pieces)]
        ys = [
            remote(both.at[0, at], both.at[1, at], y_s.at[i], y_r.at[i], to_y)
            for i, at in enumerate(cut_at)
        ]
        wide_x = both[0].astype(f32)
        square = jnp.sum(wide_x * wide_x, axis=1, keepdims=True)
        sbuf[me_d, me_t] = jnp.broadcast_to(square, (tokens, HEAD_DIM)).T[:8]
        stats = [
            remote(
                sbuf.at[me_d, me_t], sbuf.at[me_d, me_t], s_s.at[i], s_r.at[i], peer
            )
            for i, peer in enumerate(peers)
        ]
        cot_y = remote(cotf.at[me_t], cotf.at[me_t], c_s.at[0], c_r.at[0], to_y)
        cot_a = remote(cotf.at[me_t], cotf.at[me_t], c_s.at[1], c_r.at[1], to_sib)
        row = lax.broadcasted_iota(jnp.int32, (every, every), 1)
        pm[...] = (row == src_r[...]).astype(f32).astype(bf)
        xs, subs = [], []
        for i, at in enumerate(cut_at):
            ys[i].wait()
            xs.append(remote(both.at[relay, at], xbuf.at[at], x_s.at[i], x_r.at[i], to_x))
            subs.append(remote(both.at[home, at], sibd.at[at], a_s.at[i], a_r.at[i], to_sib))
        for i, at in enumerate(cut_at):
            xs[i].wait()
            subs.append(remote(xbuf.at[at], sibx.at[at], b_s.at[i], b_r.at[i], to_sib))
        for copy in stats:
            copy.wait()
        for s in range(shards):
            total = sbuf[s, 0]
            for t in range(1, feats):
                total = total + sbuf[s, t]
            scales = lax.rsqrt(total / (wide * feats) + 1e-06)
            inv_s[s] = jnp.broadcast_to(scales[:1], (HEAD_DIM, tokens)).T
        for copy in subs:
            copy.wait()

        def normalise(src, which, column):
            def step(i, carry):
                at = pl.ds(pl.multiple_of(i * 32, 32), 32)
                to = pl.ds(pl.multiple_of(which * tokens + i * 32, 32), 32)
                columns = pl.ds(pl.multiple_of(column * wide, wide), wide)
                nb[to, columns] = (
                    src[at, :].astype(f32)
                    * inv_s[which, at, :1]
                    * gain_r[me_d, :, columns]
                ).astype(bf)
                return carry

            lax.fori_loop(0, tokens // 32, step, 0)

        normalise(both.at[home], me_d, core)
        normalise(sibd, me_d, 1 - core)
        normalise(xbuf, other, core)
        normalise(sibx, other, 1 - core)

        def permute(i, carry):
            at = pl.ds(pl.multiple_of(i * 512, 512), 512)
            tile = jnp.dot(pm[...], nb[:, at], preferred_element_type=f32).astype(bf)
            nb[:, at] = tile
            blk_o[at, :] = tile.T
            return carry

        lax.fori_loop(0, half // 512, permute, 0)
        for one in loads:
            one.wait()

        def projected(which):
            rows = nb[pl.ds(pl.multiple_of(which * tokens, tokens), tokens), :]
            return jnp.concatenate(
                [jnp.dot(rows, w[...], preferred_element_type=f32) for w in (wq, wk, wv)], axis=1
            )

        jsend[...] = projected(other).astype(bf)
        swap = remote(jsend, jrecv, j_s.at[0], j_r.at[0], to_x)
        mine = remote(both.at[0], mbuf, j_s.at[1], j_r.at[1], to_x)
        own = projected(me_d)
        cot_y.wait()
        cot_b = remote(cotf.at[across], cotf.at[across], c_s.at[2], c_r.at[2], to_sib)
        cot_a.wait()
        cot_b.wait()
        slot = lax.broadcasted_iota(jnp.int32, (tokens, 1), 0) % length
        live = slot < cnt_r[...]
        d_context = None
        for q in range(feats):
            one = lax.dot_general(
                cotf[q], wo[:, q * wide : (q + 1) * wide], nt, preferred_element_type=f32
            )
            d_context = one if d_context is None else d_context + one
        d_context = jnp.where(live, d_context, 0.0).astype(bf)
        swap.wait()
        joined = (own + jrecv[...].astype(f32)).astype(bf)
        keys = joined[:, qcols : qcols + HEAD_DIM]
        values = joined[:, qcols + HEAD_DIM :]
        at_i = lax.broadcasted_iota(jnp.int32, (tokens, tokens), 0)
        at_j = lax.broadcasted_iota(jnp.int32, (tokens, tokens), 1)
        mask = (
            (at_i // length == at_j // length) & (at_j <= at_i) & (at_j % length < cnt_r[...])
        )
        contexts = []
        for h in range(heads):
            cols = slice(h * HEAD_DIM, (h + 1) * HEAD_DIM)
            rows = slice(h * tokens, (h + 1) * tokens)
            query, d_ctx = joined[:, cols], d_context[:, cols]
            score = lax.dot_general(query, keys, nt, preferred_element_type=f32) * scale
            expo = jnp.where(mask, jnp.exp(jnp.where(mask, score, 0.0)), 0.0)
            soft = expo / jnp.sum(expo, axis=1, keepdims=True)
            short = soft.astype(bf)
            contexts.append(jnp.dot(short, values, preferred_element_type=f32).astype(bf))
            d_soft = lax.dot_general(d_ctx, values, nt, preferred_element_type=f32)
            d_score = soft * (d_soft - jnp.sum(d_soft * soft, axis=1, keepdims=True)) * scale
            d_score = d_score.astype(bf)
            d_o[:, cols] = jnp.dot(d_score, keys, preferred_element_type=f32).astype(bf)
            qs[rows], dcs[rows], ws[rows], dss[rows] = query, d_ctx, short, d_score
        d_o[:, qcols : qcols + HEAD_DIM] = lax.dot_general(
            dss[...], qs[...], tn, preferred_element_type=f32
        ).astype(bf)
        d_o[:, qcols + HEAD_DIM :] = lax.dot_general(
            ws[...], dcs[...], tn, preferred_element_type=f32
        ).astype(bf)
        context = jnp.concatenate(contexts, axis=1)
        for q in range(feats):
            part_o[q] = jnp.dot(
                context, wo[:, q * wide : (q + 1) * wide], preferred_element_type=f32
            ).astype(bf)
        mine.wait()
        pick = pl.ds(pl.multiple_of(me_d * tokens, tokens), tokens)
        rest = pl.ds(pl.multiple_of(other * tokens, tokens), tokens)
        mine_o[...] = (
            jnp.dot(pm[pick, pick], both[0], preferred_element_type=f32)
            + jnp.dot(pm[pick, rest], mbuf[...], preferred_element_type=f32)
        ).astype(bf)

    dma = pltpu.SemaphoreType.DMA
    vmem, hbm = pl.BlockSpec(memory_space=pltpu.VMEM), pl.BlockSpec(memory_space=pl.ANY)
    tall = heads * tokens
    return pl.pallas_call(
        kernel,
        out_shape=[
            jax.ShapeDtypeStruct((half, every), bf),
            jax.ShapeDtypeStruct((tokens, join), bf),
            jax.ShapeDtypeStruct((feats, tokens, wide), bf),
            jax.ShapeDtypeStruct((tokens, wide), bf),
        ],
        in_specs=[hbm] * 2 + [vmem] * 3 + [hbm] * 4,
        out_specs=[vmem] * 4,
        scratch_shapes=[
            pltpu.VMEM(weights[0].shape, bf),
            pltpu.VMEM(weights[1].shape, bf),
            pltpu.VMEM(weights[2].shape, bf),
            pltpu.VMEM(w_out.shape, bf),
            pltpu.VMEM((2, tokens, wide), bf),
            pltpu.VMEM((tokens, wide), bf),
            pltpu.VMEM((tokens, wide), bf),
            pltpu.VMEM((tokens, wide), bf),
            pltpu.VMEM((tokens, wide), bf),
            pltpu.VMEM((feats, tokens, wide), bf),
            pltpu.VMEM((shards, feats, 8, tokens), f32),
            pltpu.VMEM((shards, tokens, HEAD_DIM), f32),
            pltpu.VMEM((every, half), bf),
            pltpu.VMEM((every, every), bf),
            pltpu.VMEM((tokens, join), bf),
            pltpu.VMEM((tokens, join), bf),
            pltpu.VMEM((tall, HEAD_DIM), bf),
            pltpu.VMEM((tall, HEAD_DIM), bf),
            pltpu.VMEM((tall, tokens), bf),
            pltpu.VMEM((tall, tokens), bf),
            dma((6,)),
            dma((shards * feats - 1,)),
            dma((shards * feats - 1,)),
        ]
        + [dma((pieces,))] * 8
        + [dma((3,)), dma((3,)), dma((2,)), dma((2,))],
        compiler_params=pltpu.CompilerParams(
            collective_id=0, has_side_effects=True, vmem_limit_bytes=60 * 2**20
        ),
        cost_estimate=pl.CostEstimate(
            flops=40_000_000_000, bytes_accessed=2 * (join + qcols) * half, transcendentals=0
        ),
        name="front",
    )(
        own_x,
        own_cot,
        gain.reshape(shards, 1, half),
        source.reshape(-1, 1),
        counts.reshape(-1, 1),
        *weights,
        w_out,
    )


def finish(
    hidden, gain, weights, w_out, cache_keys, cache_values, lengths, reward_vec,
    order, block, d_own, part, mine,
):
    shards, feats = lax.axis_size("dp"), lax.axis_size("tp")
    groups = lax.axis_size("grp")
    half, every = block.shape
    tokens, wide_t = mine.shape
    share = half // feats
    rows, dim = hidden.shape
    slots = cache_keys.shape[1]
    wide = dim // feats
    per = feats // shards
    heads = weights[0].shape[1] // HEAD_DIM
    join = sum(w.shape[1] for w in weights)
    qcols = weights[0].shape[1]
    scale = 1.0 / HEAD_DIM**0.5
    tall = heads * rows
    extra = HEAD_DIM
    dims = (((1,), (1,)), ((), ()))

    def kernel(
        hid, gain_r, len_r, rvec, ord_r,
        ck_h, cv_h, wq_h, wk_h, wv_h, wo_h, blk_h, d_h, part_h, mine_h,
        dec_o, adv_o, all_o, layer_o, alln, alld,
        wq, wk, wv, wo, ck, cv, bv, dv, pt, mt, sibp, ysend, yrecv, abuf,
        st, nsend, nbuf, psend, pbuf, osend, obuf, snew, kn, vn, rbuf,
        lsem, hs, hr, ps, pr, os_, or_, ss, sr, rs, rr,
        zs, zr, ks, kr, xs, xr, ls, lr, gs, gr,
    ):
        me_g, me_d, me_t = lax.axis_index("grp"), lax.axis_index("dp"), lax.axis_index("tp")
        core = lax.rem(me_t, 2)
        sib = me_t + 1 - 2 * core
        across = lax.rem(me_t + 2, feats)
        above, below = lax.rem(me_g + 1, groups), lax.rem(me_g + groups - 1, groups)
        loads = []
        for at, (src, dst) in enumerate(
            (
                (blk_h, bv), (d_h, dv), (wq_h, wq), (wk_h, wk), (wv_h, wv), (ck_h, ck), (cv_h, cv),
                (wo_h, wo), (part_h, pt), (mine_h, mt),
            )
        ):
            loads.append(pltpu.make_async_copy(src, dst, lsem.at[at]))
            loads[-1].start()
        barrier = pltpu.get_barrier_semaphore()
        for off in range(1, shards):
            pl.semaphore_signal(
                barrier, inc=1, device_id={"dp": lax.rem(me_d + off, shards)}, device_id_type=MESH
            )
        for off in range(1, feats):
            pl.semaphore_signal(
                barrier, inc=1, device_id={"tp": lax.rem(me_t + off, feats)}, device_id_type=MESH
            )
        for off in range(1, groups):
            pl.semaphore_signal(
                barrier, inc=1, device_id={"grp": lax.rem(me_g + off, groups)}, device_id_type=MESH
            )
        for q in range(feats):
            st[q] = hid[:, q * wide : (q + 1) * wide]
        kn[...] = jnp.zeros_like(kn)
        vn[...] = jnp.zeros_like(vn)
        lens = jnp.concatenate([len_r[...]] * heads, axis=0)
        row_c = lax.broadcasted_iota(jnp.int32, (tall, rows * slots), 0) % rows
        col_c = lax.broadcasted_iota(jnp.int32, (tall, rows * slots), 1)
        live_c = (col_c // slots == row_c) & (col_c % slots < lens)
        row_n = lax.broadcasted_iota(jnp.int32, (tall, extra), 0) % rows
        col_n = lax.broadcasted_iota(jnp.int32, (tall, extra), 1)
        pl.semaphore_wait(barrier, shards - 1 + feats - 1 + groups - 1)
        loads[0].wait()
        loads[1].wait()
        keep = [
            pltpu.make_async_copy(bv, alln.at[me_g], lsem.at[10]),
            pltpu.make_async_copy(dv, alld.at[me_g, me_d], lsem.at[11]),
        ]
        for copy in keep:
            copy.start()

        def remote(src, dst, send, recv, target):
            return pltpu.make_async_remote_copy(
                src_ref=src,
                dst_ref=dst,
                send_sem=send,
                recv_sem=recv,
                device_id=target,
                device_id_type=MESH,
            )

        def part_of(which):
            return pl.ds(pl.multiple_of(which * share, share), share)

        def hop(item, up, h, at, first):
            where = {"grp": above if up else below}
            sems = zs.at[item, int(up), h - 1], zr.at[item, int(up), h - 1]
            if item == 0:
                src = bv.at[part_of(me_t)] if first else alln.at[at, part_of(me_t)]
                return remote(src, alln.at[at, part_of(me_t)], *sems, where)
            src = dv if first else alld.at[at, me_d]
            return remote(src, alld.at[at, me_d], *sems, where)

        def send_hop(item, h):
            for up in (True, False):
                at = me_g - h + 1 if up else me_g + h - 1
                ok = (at >= 0) & (me_g + 1 < groups) if up else (at < groups) & (me_g > 0)

                @pl.when(ok)
                def _():
                    hop(item, up, h, at, h == 1).start()

        def end_hop(item, h):
            for up in (True, False):
                at = me_g - h + 1 if up else me_g + h - 1
                ok = (at >= 0) & (me_g + 1 < groups) if up else (at < groups) & (me_g > 0)

                @pl.when(ok)
                def _():
                    hop(item, up, h, at, h == 1).wait_send()

        def arrivals(h):
            for up in (True, False):
                at = me_g - h if up else me_g + h
                yield up, at, (at >= 0) if up else (at < groups)

        def spread(up, h, at):
            sems = [(ks.at[int(up), h - 1, i], kr.at[int(up), h - 1, i]) for i in range(3)]
            ours, theirs = part_of(me_t), part_of(across)
            return (
                remote(alln.at[at, ours], alln.at[at, ours], *sems[0], {"tp": across}),
                remote(alln.at[at, ours], alln.at[at, ours], *sems[1], {"tp": sib}),
                remote(alln.at[at, theirs], alln.at[at, theirs], *sems[2], {"tp": sib}),
            )

        def cross(up, h, at):
            src = alld.at[at, me_d]
            return remote(src, src, xs.at[int(up), h - 1], xr.at[int(up), h - 1], {"dp": 1 - me_d})

        def got_block(h):
            for up, at, ok in arrivals(h):

                @pl.when(ok)
                def _():
                    hop(0, up, h, at, False).wait_recv()

            if h + 1 < groups:
                send_hop(0, h + 1)
            for up, at, ok in arrivals(h):

                @pl.when(ok)
                def _():
                    first, second, _ = spread(up, h, at)
                    first.start()
                    second.start()

        def pass_on(h):
            for up, at, ok in arrivals(h):

                @pl.when(ok)
                def _():
                    first, _, third = spread(up, h, at)
                    first.wait_recv()
                    third.start()

        def got_d(h):
            for up, at, ok in arrivals(h):

                @pl.when(ok)
                def _():
                    hop(1, up, h, at, False).wait_recv()

            if h + 1 < groups:
                send_hop(1, h + 1)
            for up, at, ok in arrivals(h):

                @pl.when(ok)
                def _():
                    cross(up, h, at).start()

        send_hop(0, 1)
        send_hop(1, 1)
        own_d = remote(dv, alld.at[me_g, me_d], xs.at[0, groups - 1], xr.at[0, groups - 1], {"dp": 1 - me_d})
        loads = loads[2:]

        for step in range(STEPS):
            total = jnp.zeros((rows, 1), jnp.float32)
            for q in range(feats):
                cell = st[q].astype(jnp.float32)
                total = total + jnp.sum(cell * cell, axis=1, keepdims=True)
            inv = lax.rsqrt(total / dim + 1e-06)
            for q in range(feats):
                nsend[step, q] = (
                    st[q].astype(jnp.float32) * inv * gain_r[:, q * wide : (q + 1) * wide]
                ).astype(jnp.bfloat16)
            copies = []
            for off in range(1, shards):
                peer = lax.rem(me_d + off, shards)
                copies.append(
                    pltpu.make_async_remote_copy(
                        src_ref=nsend.at[step, pl.ds(peer * per, per)],
                        dst_ref=nbuf.at[step, me_d],
                        send_sem=hs.at[step, off - 1],
                        recv_sem=hr.at[step, off - 1],
                        device_id={"dp": peer},
                        device_id_type=MESH,
                    )
                )
                copies[-1].start()
            nbuf[step, me_d] = nsend[step, pl.ds(me_d * per, per)]
            if step == 0:
                for one in loads[:3]:
                    one.wait()
            for copy in copies:
                copy.wait()
            parts = []
            for w in (wq, wk, wv):
                acc = None
                for q in range(per):
                    left = jnp.concatenate([nbuf[step, s, q] for s in range(shards)], axis=0)
                    one = jnp.dot(
                        left, w[q * wide : (q + 1) * wide], preferred_element_type=jnp.float32
                    )
                    acc = one if acc is None else acc + one
                parts.append(acc)
            part = jnp.concatenate(parts, axis=1)
            for s in range(shards):
                psend[step, s] = part[s * rows : (s + 1) * rows]
            copies = []
            for off in range(1, shards):
                peer = lax.rem(me_d + off, shards)
                copies.append(
                    pltpu.make_async_remote_copy(
                        src_ref=psend.at[step, peer],
                        dst_ref=pbuf.at[step, me_d],
                        send_sem=ps.at[step, off - 1],
                        recv_sem=pr.at[step, off - 1],
                        device_id={"dp": peer},
                        device_id_type=MESH,
                    )
                )
                copies[-1].start()
            pbuf[step, me_d] = psend[step, me_d]
            if step == 0:
                own_d.start()
                for one in loads[3:]:
                    one.wait()
                swaps = [
                    remote(
                        pt.at[2 * s + 1 - core], sibp.at[s], ls.at[s], lr.at[s], {"tp": sib}
                    )
                    for s in range(feats // 2)
                ]
                for copy in swaps:
                    copy.start()
            if step == 1:
                got_d(1)
                pass_on(1)
            for copy in copies:
                copy.wait()
            joined = pbuf[step, 0]
            for s in range(1, shards):
                joined = joined + pbuf[step, s]
            joined = joined.astype(jnp.bfloat16)
            query = jnp.concatenate(
                [joined[:, h * HEAD_DIM : (h + 1) * HEAD_DIM] for h in range(heads)], axis=0
            )
            kn[step * rows : (step + 1) * rows] = joined[:, qcols : qcols + HEAD_DIM]
            vn[step * rows : (step + 1) * rows] = joined[:, qcols + HEAD_DIM :]
            score_c = (
                lax.dot_general(query, ck[...], dims, preferred_element_type=jnp.float32) * scale
            )
            score_n = (
                lax.dot_general(query, kn[...], dims, preferred_element_type=jnp.float32) * scale
            )
            expo_c = jnp.where(live_c, jnp.exp(jnp.where(live_c, score_c, 0.0)), 0.0)
            live_n = (col_n % rows == row_n) & (col_n < (step + 1) * rows)
            expo_n = jnp.where(live_n, jnp.exp(jnp.where(live_n, score_n, 0.0)), 0.0)
            denom = jnp.sum(expo_c, axis=1, keepdims=True) + jnp.sum(expo_n, axis=1, keepdims=True)
            soft_c = (expo_c / denom).astype(jnp.bfloat16)
            soft_n = (expo_n / denom).astype(jnp.bfloat16)
            ctx = (
                jnp.dot(soft_c, cv[...], preferred_element_type=jnp.float32)
                + jnp.dot(soft_n, vn[...], preferred_element_type=jnp.float32)
            ).astype(jnp.bfloat16)
            context = jnp.concatenate(
                [ctx[h * rows : (h + 1) * rows] for h in range(heads)], axis=1
            )
            for q in range(feats):
                osend[step, q] = jnp.dot(
                    context, wo[:, q * wide : (q + 1) * wide], preferred_element_type=jnp.float32
                ).astype(jnp.bfloat16)
            copies = []
            for off in range(1, feats):
                peer = lax.rem(me_t + off, feats)
                copies.append(
                    pltpu.make_async_remote_copy(
                        src_ref=osend.at[step, peer],
                        dst_ref=obuf.at[step, me_t],
                        send_sem=os_.at[step, off - 1],
                        recv_sem=or_.at[step, off - 1],
                        device_id={"tp": peer},
                        device_id_type=MESH,
                    )
                )
                copies[-1].start()
            obuf[step, me_t] = osend[step, me_t]
            if step == 1:
                got_block(2)
            for copy in copies:
                copy.wait()
            acc = st[me_t].astype(jnp.float32)
            for s in range(feats):
                acc = acc + obuf[step, s].astype(jnp.float32)
            snew[step, me_t] = acc.astype(jnp.bfloat16)
            copies = []
            for off in range(1, feats):
                peer = lax.rem(me_t + off, feats)
                copies.append(
                    pltpu.make_async_remote_copy(
                        src_ref=snew.at[step, me_t],
                        dst_ref=snew.at[step, me_t],
                        send_sem=ss.at[step, off - 1],
                        recv_sem=sr.at[step, off - 1],
                        device_id={"tp": peer},
                        device_id_type=MESH,
                    )
                )
                copies[-1].start()
            for copy in copies:
                copy.wait()
            for q in range(feats):
                st[q] = snew[step, q]
            if step == 0:
                got_block(1)
                for copy in swaps:
                    copy.wait()
                theirs = lax.rem(me_t // 2 + 1, 2)
                ysend[...] = (
                    pt[2 * theirs + core].astype(jnp.float32)
                    + sibp[theirs].astype(jnp.float32)
                ).astype(jnp.bfloat16)
                swap_y = remote(ysend, yrecv, ls.at[2], lr.at[2], {"tp": across})
                swap_y.start()
            else:
                got_d(2)
                pass_on(2)

        reward = jnp.zeros((rows, 1), jnp.float32)
        for q in range(feats):
            dec_o[:, q * wide : (q + 1) * wide] = st[q]
            reward = reward + jnp.sum(
                st[q].astype(jnp.float32) * rvec[:, q * wide : (q + 1) * wide],
                axis=1,
                keepdims=True,
            )
        rbuf[me_d] = jnp.broadcast_to(reward, (rows, HEAD_DIM))
        copies = []
        for off in range(1, shards):
            peer = lax.rem(me_d + off, shards)
            copies.append(
                pltpu.make_async_remote_copy(
                    src_ref=rbuf.at[me_d],
                    dst_ref=rbuf.at[me_d],
                    send_sem=rs.at[off - 1],
                    recv_sem=rr.at[off - 1],
                    device_id={"dp": peer},
                    device_id_type=MESH,
                )
            )
            copies[-1].start()
        for copy in copies:
            copy.wait()
        count = shards * rows
        every_r = jnp.concatenate([rbuf[s] for s in range(shards)], axis=0)
        mean = jnp.sum(every_r, axis=0, keepdims=True) / count
        spread_r = jnp.sum(every_r * every_r, axis=0, keepdims=True) / count - mean * mean
        adv = (every_r - mean) / jnp.sqrt(spread_r + 1e-05)
        adv_o[...] = adv
        turn = lax.broadcasted_iota(jnp.int32, (count, count), 1) == ord_r[...]
        abuf[me_g] = jnp.dot(
            turn.astype(jnp.float32).astype(jnp.bfloat16),
            adv.astype(jnp.bfloat16),
            preferred_element_type=jnp.float32,
        ).astype(jnp.bfloat16)
        advs = []
        for off in range(1, groups):
            advs.append(
                remote(
                    abuf.at[me_g],
                    abuf.at[me_g],
                    gs.at[off - 1],
                    gr.at[off - 1],
                    {"grp": lax.rem(me_g + off, groups)},
                )
            )
            advs[-1].start()
        swap_y.wait()
        layer_o[...] = (
            mt[...].astype(jnp.float32)
            + pt[me_t].astype(jnp.float32)
            + sibp[me_t // 2].astype(jnp.float32)
            + yrecv[...].astype(jnp.float32)
        ).astype(jnp.bfloat16)
        last = groups - 1
        got_block(last)
        got_d(last)
        pass_on(last)
        for copy in advs:
            copy.wait()
        all_o[...] = abuf[...]
        for copy in keep:
            copy.wait()
        own_d.wait()
        for h in range(1, groups):
            for item in range(2):
                end_hop(item, h)
            for up, at, ok in arrivals(h):

                @pl.when(ok)
                def _():
                    first, second, third = spread(up, h, at)
                    first.wait_send()
                    second.wait()
                    third.wait()
                    cross(up, h, at).wait()

    bf, f32 = jnp.bfloat16, jnp.float32
    dma = pltpu.SemaphoreType.DMA
    vmem, hbm = pl.BlockSpec(memory_space=pltpu.VMEM), pl.BlockSpec(memory_space=pl.ANY)
    flops = 2 * STEPS * dim * (join + qcols) * rows * 2
    return pl.pallas_call(
        kernel,
        out_shape=[
            jax.ShapeDtypeStruct((rows, dim), bf),
            jax.ShapeDtypeStruct((shards * rows, HEAD_DIM), f32),
            jax.ShapeDtypeStruct((groups, shards * rows, HEAD_DIM), bf),
            jax.ShapeDtypeStruct((tokens, wide), bf),
            jax.ShapeDtypeStruct((groups, half, every), bf),
            jax.ShapeDtypeStruct((groups, shards, tokens, join), bf),
        ],
        in_specs=[vmem] * 5 + [hbm] * 10,
        out_specs=[vmem] * 4 + [hbm] * 2,
        scratch_shapes=[
            pltpu.VMEM(weights[0].shape, bf),
            pltpu.VMEM(weights[1].shape, bf),
            pltpu.VMEM(weights[2].shape, bf),
            pltpu.VMEM(w_out.shape, bf),
            pltpu.VMEM((rows * slots, HEAD_DIM), bf),
            pltpu.VMEM((rows * slots, HEAD_DIM), bf),
            pltpu.VMEM((half, every), bf),
            pltpu.VMEM((tokens, join), bf),
            pltpu.VMEM((feats, tokens, wide), bf),
            pltpu.VMEM((tokens, wide), bf),
            pltpu.VMEM((feats // 2, tokens, wide), bf),
            pltpu.VMEM((tokens, wide), bf),
            pltpu.VMEM((tokens, wide), bf),
            pltpu.VMEM((groups, shards * rows, HEAD_DIM), bf),
            pltpu.VMEM((feats, rows, wide), bf),
            pltpu.VMEM((STEPS, feats, rows, wide), bf),
            pltpu.VMEM((STEPS, shards, per, rows, wide), bf),
            pltpu.VMEM((STEPS, shards, rows, join), f32),
            pltpu.VMEM((STEPS, shards, rows, join), f32),
            pltpu.VMEM((STEPS, feats, rows, wide), bf),
            pltpu.VMEM((STEPS, feats, rows, wide), bf),
            pltpu.VMEM((STEPS, feats, rows, wide), bf),
            pltpu.VMEM((extra, HEAD_DIM), bf),
            pltpu.VMEM((extra, HEAD_DIM), bf),
            pltpu.VMEM((shards, rows, HEAD_DIM), f32),
            dma((12,)),
            dma((STEPS, shards - 1)),
            dma((STEPS, shards - 1)),
            dma((STEPS, shards - 1)),
            dma((STEPS, shards - 1)),
            dma((STEPS, feats - 1)),
            dma((STEPS, feats - 1)),
            dma((STEPS, feats - 1)),
            dma((STEPS, feats - 1)),
            dma((shards - 1,)),
            dma((shards - 1,)),
            dma((2, 2, groups - 1)),
            dma((2, 2, groups - 1)),
            dma((2, groups - 1, 3)),
            dma((2, groups - 1, 3)),
            dma((2, groups)),
            dma((2, groups)),
            dma((3,)),
            dma((3,)),
            dma((groups - 1,)),
            dma((groups - 1,)),
        ],
        compiler_params=pltpu.CompilerParams(
            collective_id=1, has_side_effects=True, vmem_limit_bytes=60 * 2**20
        ),
        cost_estimate=pl.CostEstimate(
            flops=40_000_000_000, bytes_accessed=2 * (join + qcols) * dim, transcendentals=0
        ),
        name="finish",
    )(
        hidden,
        gain.reshape(1, -1),
        lengths.reshape(-1, 1),
        reward_vec.reshape(1, -1),
        order.reshape(-1, 1),
        cache_keys.reshape(rows * slots, -1),
        cache_values.reshape(rows * slots, -1),
        *weights,
        w_out,
        block,
        d_own,
        part,
        mine,
    )


def gradients(length, blocks, every_d, advantages, weights):
    groups, half, every = blocks.shape
    join = every_d.shape[-1]
    rows = advantages.shape[1]
    cuts = [w.shape[1] for w in weights]
    tile = 256
    bf, f32 = jnp.bfloat16, jnp.float32

    def kernel(n_r, d_r, a_r, q_o, k_o, v_o, ds):
        @pl.when(pl.program_id(0) == 0)
        def _():
            at = lax.broadcasted_iota(jnp.int32, (every, rows), 0) // length
            repeat = (at == lax.broadcasted_iota(jnp.int32, (every, rows), 1)).astype(f32)
            for g in range(groups):
                adv = jnp.dot(repeat.astype(bf), a_r[g], preferred_element_type=f32)
                for s in range(0, join, HEAD_DIM):
                    ds[g, :, s : s + HEAD_DIM] = (
                        adv * d_r[g, :, s : s + HEAD_DIM].astype(f32)
                    ).astype(bf)

        total = None
        for g in range(groups):
            one = jnp.dot(n_r[g], ds[g], preferred_element_type=f32)
            total = one if total is None else total + one
        q_o[...] = total[:, : cuts[0]]
        k_o[...] = total[:, cuts[0] : cuts[0] + cuts[1]]
        v_o[...] = total[:, cuts[0] + cuts[1] :]

    return pl.pallas_call(
        kernel,
        grid=(half // tile,),
        out_shape=[jax.ShapeDtypeStruct((half, cut), f32) for cut in cuts],
        in_specs=[
            pl.BlockSpec((groups, tile, every), lambda i: (0, i, 0)),
            pl.BlockSpec((groups, every, join), lambda i: (0, 0, 0)),
            pl.BlockSpec((groups, rows, HEAD_DIM), lambda i: (0, 0, 0)),
        ],
        out_specs=[pl.BlockSpec((tile, cut), lambda i: (i, 0)) for cut in cuts],
        scratch_shapes=[pltpu.VMEM((groups, every, join), bf)],
        compiler_params=pltpu.CompilerParams(dimension_semantics=("arbitrary",)),
        cost_estimate=pl.CostEstimate(
            flops=2 * groups * every * half * join,
            bytes_accessed=2 * groups * every * (half + join) + 4 * half * join,
            transcendentals=0,
        ),
        name="gradients",
    )(blocks, every_d, advantages)


def on_device(
    hidden_last,
    gain,
    w_query,
    w_key,
    w_value,
    w_out,
    cache_keys,
    cache_values,
    cache_lengths,
    reward_vec,
    response_counts,
    assignment,
    responses,
    cotangent,
):
    shards = lax.axis_size("dp")
    myself = lax.axis_index("dp")
    weights = (w_query, w_key, w_value)
    rows_dev, length, _ = responses.shape
    tokens = rows_dev * length
    group_rows = assignment.shape[0]

    positions = jnp.arange(group_rows, dtype=jnp.int32)
    place = assignment * rows_dev + exclusive_rank(assignment, shards)
    order = jnp.sum(jnp.where(place[None, :] == positions[:, None], positions[None, :], 0), axis=1)
    slots = jnp.arange(length, dtype=jnp.int32)
    source = (order[:, None] * length + slots[None, :]).reshape(-1)
    chosen = lax.dynamic_slice_in_dim(order, myself * rows_dev, rows_dev)
    wanted = chosen[:, None] == positions[None, :]
    counts = jnp.sum(jnp.where(wanted, response_counts[None, :], 0), axis=1)

    block, d_own, part, mine = front(
        length,
        responses.reshape(tokens, -1),
        cotangent.reshape(tokens, -1),
        gain,
        source,
        jnp.repeat(counts, length),
        weights,
        w_out,
    )
    state, every_adv, all_adv, layer, blocks, every_d = finish(
        hidden_last,
        gain,
        weights,
        w_out,
        cache_keys,
        cache_values,
        cache_lengths,
        reward_vec,
        order,
        block,
        d_own,
        part,
        mine,
    )
    advantage = lax.dynamic_slice_in_dim(every_adv[:, 0], myself * rows_dev, rows_dev)
    grads = gradients(
        length, blocks, every_d.reshape(blocks.shape[0], shards * tokens, -1), all_adv, weights
    )
    return (state, advantage, layer.reshape(rows_dev, length, -1), *grads)


def solution(mesh):
    small = mesh.shape["dp"] == 2 and mesh.shape["tp"] == 4
    return jax.shard_map(
        on_device if small else on_device_plain,
        mesh=mesh,
        in_specs=(
            P(("grp", "dp"), None),
            P(),
            P("dp", "tp"),
            P("dp", "tp"),
            P("dp", "tp"),
            P("tp", None),
            P(("grp", "dp"), None, "tp"),
            P(("grp", "dp"), None, "tp"),
            P(("grp", "dp")),
            P(),
            P("grp"),
            P("grp"),
            P(("grp", "dp"), None, "tp"),
            P(("grp", "dp"), None, "tp"),
        ),
        out_specs=(
            P(("grp", "dp"), None),
            P(("grp", "dp")),
            P(("grp", "dp"), None, "tp"),
            P("dp", "tp"),
            P("dp", "tp"),
            P("dp", "tp"),
        ),
        check_vma=False,
    )
```

```python
import jax
import jax.numpy as jnp
from jax import lax
from jax.experimental import pallas as pl
from jax.experimental.pallas import tpu as pltpu
from jax.sharding import PartitionSpec as P

HEAD_DIM = 128
STEPS = 2
MESH = pl.DeviceIdType.MESH


def norm_rows(values, gain):
    wide = values.astype(jnp.float32)
    meansq = jnp.mean(wide * wide, axis=-1, keepdims=True)
    return (wide * lax.rsqrt(meansq + 1e-06) * gain).astype(jnp.bfloat16)


def rounded(values):
    return lax.optimization_barrier(values.astype(jnp.bfloat16)).astype(jnp.float32)


def decode_attend(query, cache_k, cache_v, lengths, new_k, new_v):
    rows_n = query.shape[0]
    slots = cache_k.shape[1]
    kv_n = cache_k.shape[2] // HEAD_DIM
    per_kv = query.shape[1] // cache_k.shape[2]
    scale = 1.0 / HEAD_DIM**0.5
    quer = query.reshape(rows_n, kv_n, per_kv, HEAD_DIM)
    keys_c = cache_k.reshape(rows_n, slots, kv_n, HEAD_DIM)
    vals_c = cache_v.reshape(rows_n, slots, kv_n, HEAD_DIM)
    keys_n = new_k.reshape(rows_n, -1, kv_n, HEAD_DIM)
    vals_n = new_v.reshape(rows_n, -1, kv_n, HEAD_DIM)
    score_c = (
        jnp.einsum("rkgd,rckd->rkgc", quer, keys_c, preferred_element_type=jnp.float32) * scale
    )
    score_n = (
        jnp.einsum("rkgd,rnkd->rkgn", quer, keys_n, preferred_element_type=jnp.float32) * scale
    )
    live = (jnp.arange(slots, dtype=jnp.int32)[None, :] < lengths[:, None])[:, None, None, :]
    score_c = jnp.where(live, score_c, -1e30)
    scores = jnp.concatenate([score_c, score_n], axis=-1)
    expo = jnp.exp(scores)
    weights = (expo / jnp.sum(expo, axis=-1, keepdims=True)).astype(jnp.bfloat16)
    context = jnp.einsum(
        "rkgc,rckd->rkgd", weights[..., :slots], vals_c, preferred_element_type=jnp.float32
    )
    context = context + jnp.einsum(
        "rkgn,rnkd->rkgd", weights[..., slots:], vals_n, preferred_element_type=jnp.float32
    )
    return context.reshape(rows_n, -1).astype(jnp.bfloat16)


def attend(query, keys, values, counts):
    rows_n = counts.shape[0]
    tokens = query.shape[0]
    length = tokens // rows_n
    kv_n = keys.shape[1] // HEAD_DIM
    per_kv = query.shape[1] // keys.shape[1]
    scale = 1.0 / HEAD_DIM**0.5
    quer = query.reshape(rows_n, length, kv_n, per_kv, HEAD_DIM).astype(jnp.float32)
    keyf = keys.reshape(rows_n, length, kv_n, HEAD_DIM).astype(jnp.float32)
    valf = values.reshape(rows_n, length, kv_n, HEAD_DIM).astype(jnp.float32)
    scores = jnp.einsum("rikgd,rjkd->rkgij", quer, keyf) * scale
    slot = jnp.arange(length, dtype=jnp.int32)
    causal = (slot[None, :] <= slot[:, None])[None, :, :]
    inside = slot[None, None, :] < counts[:, None, None]
    mask = (causal & inside)[:, None, None, :, :]
    scores = jnp.where(mask, scores, -1e30)
    expo = jnp.exp(scores)
    weights = (
        (expo / jnp.sum(expo, axis=-1, keepdims=True)).astype(jnp.bfloat16).astype(jnp.float32)
    )
    context = jnp.einsum("rkgij,rjkd->rikgd", weights, valf)
    return context.reshape(tokens, -1).astype(jnp.bfloat16)


def slot_valid(counts, length):
    slot = jnp.arange(length, dtype=jnp.int32)
    return (slot[None, :] < counts[:, None]).reshape(-1)


def exclusive_rank(labels, classes):
    onehot = (labels[:, None] == jnp.arange(classes, dtype=jnp.int32)[None, :]).astype(jnp.int32)
    return jnp.sum((jnp.cumsum(onehot, axis=0) - onehot) * onehot, axis=1)


def exchange(axis, ident, gathers=(), swaps=()):
    members = lax.axis_size(axis)
    items = tuple(gathers) + tuple(swaps)
    total = len(items)

    def kernel(*refs):
        ins, outs = refs[:total], refs[total : 2 * total]
        send_sem, recv_sem, own_sem = refs[2 * total :]
        me = lax.axis_index(axis)
        peers = [lax.rem(me + off, members) for off in range(1, members)]
        barrier = pltpu.get_barrier_semaphore()
        for peer in peers:
            pl.semaphore_signal(
                barrier, inc=1, device_id={axis: peer}, device_id_type=pl.DeviceIdType.MESH
            )
        pl.semaphore_wait(barrier, members - 1)
        copies = []
        for at, peer in enumerate(peers):
            for which in range(total):
                source = ins[which] if which < len(gathers) else ins[which].at[peer]
                copy = pltpu.make_async_remote_copy(
                    src_ref=source,
                    dst_ref=outs[which].at[me],
                    send_sem=send_sem.at[which * (members - 1) + at],
                    recv_sem=recv_sem.at[which * (members - 1) + at],
                    device_id={axis: peer},
                    device_id_type=pl.DeviceIdType.MESH,
                )
                copy.start()
                copies.append(copy)
        for which in range(total):
            source = ins[which] if which < len(gathers) else ins[which].at[me]
            copy = pltpu.make_async_copy(source, outs[which].at[me], own_sem.at[which])
            copy.start()
            copies.append(copy)
        for copy in copies:
            copy.wait()

    shapes = [(members,) + item.shape for item in gathers] + [item.shape for item in swaps]
    sent = sum(
        2 * item.size * (members if at < len(gathers) else 1) for at, item in enumerate(items)
    )
    return pl.pallas_call(
        kernel,
        out_shape=[jax.ShapeDtypeStruct(sh, item.dtype) for sh, item in zip(shapes, items)],
        in_specs=[pl.BlockSpec(memory_space=pltpu.VMEM)] * total,
        out_specs=[pl.BlockSpec(memory_space=pltpu.VMEM)] * total,
        scratch_shapes=[
            pltpu.SemaphoreType.DMA((total * (members - 1),)),
            pltpu.SemaphoreType.DMA((total * (members - 1),)),
            pltpu.SemaphoreType.DMA((total,)),
        ],
        compiler_params=pltpu.CompilerParams(collective_id=ident, has_side_effects=True),
        cost_estimate=pl.CostEstimate(
            flops=sent * 1000, bytes_accessed=2 * sent, transcendentals=0
        ),
        name=f"exchange_{ident}",
    )(*items)


def side_by_side(parts):
    return jnp.moveaxis(parts, 0, 1).reshape(parts.shape[1], -1)


def cut(values, members):
    return jnp.moveaxis(values.reshape(values.shape[0], members, -1), 1, 0)


def project(rows, weights):
    return jnp.concatenate(
        [jnp.dot(rows, weight, preferred_element_type=jnp.float32) for weight in weights], axis=1
    )


def split_qkv(joined, weights):
    first = weights[0].shape[1]
    second = first + weights[1].shape[1]
    return joined[:, :first], joined[:, first:second], joined[:, second:]


def on_device_plain(
    hidden_last,
    gain,
    w_query,
    w_key,
    w_value,
    w_out,
    cache_keys,
    cache_values,
    cache_lengths,
    reward_vec,
    response_counts,
    assignment,
    responses,
    cotangent,
):
    shards = lax.axis_size("dp")
    feats = lax.axis_size("tp")
    myself = lax.axis_index("dp")
    weights = (w_query, w_key, w_value)
    rows_dev, length, _ = responses.shape
    tokens = rows_dev * length
    group_rows = assignment.shape[0]

    positions = jnp.arange(group_rows, dtype=jnp.int32)
    place = assignment * rows_dev + exclusive_rank(assignment, shards)
    order = jnp.sum(jnp.where(place[None, :] == positions[:, None], positions[None, :], 0), axis=1)
    chosen = lax.dynamic_slice_in_dim(order, myself * rows_dev, rows_dev)

    (row_parts,) = exchange("tp", 0, gathers=(responses.reshape(tokens, -1),))
    own_normed = norm_rows(side_by_side(row_parts), gain)
    (block,) = exchange("dp", 1, swaps=(cut(own_normed, shards),))
    width = block.shape[-1]
    block = jnp.take(block.reshape(group_rows, length, width), order, axis=0)
    block = block.reshape(group_rows * length, width)
    share = group_rows * length // feats
    every_block = lax.all_gather(
        lax.dynamic_slice_in_dim(block, lax.axis_index("tp") * share, share),
        ("grp", "tp"),
        axis=0,
        tiled=True,
    )

    joined = project(block, weights).astype(jnp.bfloat16)
    mine_x = jnp.take(
        lax.all_gather(responses, "dp", axis=0, tiled=True), chosen, axis=0
    ).reshape(tokens, -1)
    (joined_parts,) = exchange("dp", 2, swaps=(joined.reshape(shards, tokens, -1),))
    joined = jnp.sum(joined_parts.astype(jnp.float32), axis=0).astype(jnp.bfloat16)
    query, keys, values = split_qkv(joined, weights)
    counts = jnp.take(response_counts, chosen)
    valid = slot_valid(counts, length)
    context, pull = jax.vjp(lambda a, b, c: attend(a, b, c, counts), query, keys, values)
    partial_out = jnp.dot(context, w_out, preferred_element_type=jnp.float32)
    layer = (
        mine_x.astype(jnp.float32)
        + lax.psum_scatter(
            partial_out.astype(jnp.bfloat16), "tp", scatter_dimension=1, tiled=True
        ).astype(jnp.float32)
    ).astype(jnp.bfloat16)

    local_cot = cotangent.reshape(tokens, -1) * valid.astype(jnp.bfloat16)[:, None]
    (cot_parts,) = exchange("tp", 3, gathers=(local_cot,))
    d_context = lax.dot_general(
        side_by_side(cot_parts),
        w_out,
        (((1,), (1,)), ((), ())),
        preferred_element_type=jnp.float32,
    ).astype(jnp.bfloat16)
    d_joined = jnp.concatenate(pull(d_context), axis=1)

    state = hidden_last
    keys_new = []
    values_new = []
    for step in range(STEPS):
        normed = norm_rows(state, gain)
        (pieces,) = exchange("dp", 4 + 3 * step, swaps=(cut(normed, shards),))
        part = project(pieces.reshape(group_rows, -1), weights)
        (parts,) = exchange("dp", 5 + 3 * step, swaps=(part.reshape(shards, rows_dev, -1),))
        step_q, step_k, step_v = split_qkv(
            jnp.sum(parts, axis=0).astype(jnp.bfloat16), weights
        )
        keys_new.append(step_k)
        values_new.append(step_v)
        step_context = decode_attend(
            step_q,
            cache_keys,
            cache_values,
            cache_lengths,
            jnp.stack(keys_new, 1),
            jnp.stack(values_new, 1),
        )
        step_out = jnp.dot(step_context, w_out, preferred_element_type=jnp.float32)
        (outs,) = exchange("tp", 6 + 3 * step, gathers=(step_out.astype(jnp.bfloat16),))
        state = (
            state.astype(jnp.float32) + jnp.sum(outs.astype(jnp.float32), axis=0)
        ).astype(jnp.bfloat16)
    reward = jnp.sum(state.astype(jnp.float32) * reward_vec, axis=-1, keepdims=True)
    (every_reward,) = exchange(
        "dp", 4 + 3 * STEPS, gathers=(jnp.broadcast_to(reward, (rows_dev, HEAD_DIM)),)
    )
    rewards = every_reward[:, :, 0].reshape(-1)
    mean = jnp.sum(rewards) / group_rows
    spread = jnp.sum(rewards * rewards) / group_rows - mean * mean
    every_adv = (rewards - mean) / jnp.sqrt(spread + 1e-05)
    advantage = lax.dynamic_slice_in_dim(every_adv, myself * rows_dev, rows_dev)
    my_adv = jnp.take(every_adv.astype(jnp.bfloat16), chosen).astype(jnp.float32)

    scaled = (jnp.repeat(my_adv, length)[:, None] * d_joined.astype(jnp.float32)).astype(
        jnp.bfloat16
    )
    every_d = lax.all_gather(scaled, ("grp", "dp"), axis=0, tiled=True)
    grad_q, grad_k, grad_v = (
        lax.dot_general(
            every_block, piece, (((0,), (0,)), ((), ())), preferred_element_type=jnp.float32
        )
        for piece in split_qkv(every_d, weights)
    )
    return (state, advantage, layer.reshape(rows_dev, length, -1), grad_q, grad_k, grad_v)


def main_kernel(
    length, own_x, own_cot, gain, weights, w_out, hidden, cache_keys, cache_values,
    lengths, reward_vec, assignment, response_counts,
):
    groups, shards, feats = lax.axis_size("grp"), lax.axis_size("dp"), lax.axis_size("tp")
    tokens, wide = own_x.shape
    half = weights[0].shape[0]
    every = shards * tokens
    heads = weights[0].shape[1] // HEAD_DIM
    qcols = weights[0].shape[1]
    join = sum(w.shape[1] for w in weights)
    rows, dim = hidden.shape
    count = shards * rows
    slots = cache_keys.shape[1]
    per = feats // shards
    share = half // feats
    pieces = 8
    size = tokens // pieces
    part_rows = tokens // 2
    scale = 1.0 / HEAD_DIM**0.5
    tall, deep = heads * rows, heads * tokens
    nt = (((1,), (1,)), ((), ()))
    tn = (((0,), (0,)), ((), ()))
    bf, f32, i32 = jnp.bfloat16, jnp.float32, jnp.int32

    def kernel(
        hid, gain_h, gain_w, len_r, rvec, asg_r, cnt_r,
        x_h, cot_h, wq_h, wk_h, wv_h, wo_h, ck_h, cv_h,
        dec_o, adv_o, layer_o, dsc_o, acc_o, alln,
        wq, wk, wv, wo, ck, cv,
        both, xbuf, sibd, sibx, mbuf, cotf, sbuf, inv_s, nb, bv, pm, joint, jsend, jrecv,
        qs, dcs, ws, dss, ctx_s, alld, pt, sibp, ysend, yrecv, abuf, acc, ms,
        st, nsend, nbuf, psend, pbuf, osend, obuf, snew, kn, vn, rbuf,
        lsem, s_s, s_r, y_s, y_r, x_s, x_r, a_s, a_r, b_s, b_r, c_s, c_r, j_s, j_r,
        hs, hr, ps, pr, os_, or_, ss, sr, rs, rr, zs, zr, ks, kr, xs, xr, ls, lr, gs, gr,
    ):
        me_g, me_d, me_t = lax.axis_index("grp"), lax.axis_index("dp"), lax.axis_index("tp")
        other = 1 - me_d
        core = lax.rem(me_t, 2)
        sib = me_t + 1 - 2 * core
        across = lax.rem(me_t + 2, feats)
        relay = lax.rem(me_t // 2 + me_d + 1, 2)
        home = 1 - relay
        above, below = lax.rem(me_g + 1, groups), lax.rem(me_g + groups - 1, groups)
        to_x, to_y, to_sib = {"dp": other}, {"tp": across}, {"tp": sib}

        def local(src, dst, at):
            copy = pltpu.make_async_copy(src, dst, lsem.at[at])
            copy.start()
            return copy

        def remote(src, dst, send, recv, target):
            return pltpu.make_async_remote_copy(
                src_ref=src,
                dst_ref=dst,
                send_sem=send,
                recv_sem=recv,
                device_id=target,
                device_id_type=MESH,
            )

        def sent(*args):
            copy = remote(*args)
            copy.start()
            return copy

        load_x = local(x_h, both.at[0], 0)
        load_c = local(cot_h, cotf.at[me_t], 1)
        load_w = [local(*pair, 2 + i) for i, pair in enumerate(((wq_h, wq), (wk_h, wk), (wv_h, wv)))]
        load_o = local(wo_h, wo, 5)
        load_k = [local(ck_h, ck, 6), local(cv_h, cv, 7)]
        barrier = pltpu.get_barrier_semaphore()
        peers = []
        for off in range(1, shards * feats):
            at = lax.rem(me_d * feats + me_t + off, shards * feats)
            peers.append({"dp": at // feats, "tp": lax.rem(at, feats)})
        for off in range(1, groups):
            peers.append({"grp": lax.rem(me_g + off, groups)})
        for peer in peers:
            pl.semaphore_signal(barrier, inc=1, device_id=peer, device_id_type=MESH)
        pl.semaphore_wait(barrier, len(peers))
        peers = peers[: shards * feats - 1]
        load_x.wait()

        cut_at = [pl.ds(i * size, size) for i in range(pieces)]
        wide_x = both[0].astype(f32)
        square = jnp.sum(wide_x * wide_x, axis=1, keepdims=True)
        sbuf[me_d, me_t] = jnp.broadcast_to(square, (tokens, HEAD_DIM)).T[:8]
        stats = [
            sent(sbuf.at[me_d, me_t], sbuf.at[me_d, me_t], s_s.at[i], s_r.at[i], peer)
            for i, peer in enumerate(peers)
        ]
        ysent = [
            sent(both.at[0, at], both.at[1, at], y_s.at[i], y_r.at[i], to_y)
            for i, at in enumerate(cut_at)
        ]

        def upright(line, n):
            same = lax.broadcasted_iota(i32, (n, n), 0) == lax.broadcasted_iota(i32, (n, n), 1)
            return jnp.sum(jnp.where(same, line, 0), axis=1, keepdims=True)

        label = asg_r[...]
        tall_label = upright(label, count)
        row_i = lax.broadcasted_iota(i32, (count, count), 0)
        row_j = lax.broadcasted_iota(i32, (count, count), 1)
        earlier = (label == tall_label) & (row_j < row_i)
        place = tall_label * rows + jnp.sum(
            jnp.where(earlier, 1, 0), axis=1, keepdims=True
        )
        spread_i = lax.broadcasted_iota(i32, (every, count), 0) // length
        spread = (spread_i == lax.broadcasted_iota(i32, (every, count), 1)).astype(f32).astype(bf)

        def per_token(column):
            broad = jnp.broadcast_to(column.astype(f32), (count, HEAD_DIM)).astype(bf)
            return jnp.dot(spread, broad, preferred_element_type=f32)

        slot_e = lax.broadcasted_iota(i32, (every, 1), 0) % length
        at_token = (per_token(place)[:, :1] + 0.5).astype(i32) * length + slot_e
        column_e = lax.broadcasted_iota(i32, (every, every), 1)
        pm[...] = (column_e == at_token).astype(f32).T.astype(bf)
        count_e = per_token(upright(cnt_r[...], count)).astype(bf)
        pick = pl.ds(pl.multiple_of(me_d * tokens, tokens), tokens)
        rest = pl.ds(pl.multiple_of(other * tokens, tokens), tokens)
        count_t = (
            jnp.dot(pm[pick, :], count_e, preferred_element_type=f32)[:, :1] + 0.5
        ).astype(i32)

        for q in range(feats):
            st[q] = hid[:, q * wide : (q + 1) * wide]
        kn[...] = jnp.zeros_like(kn)
        vn[...] = jnp.zeros_like(vn)

        lens = jnp.concatenate([upright(len_r[...], rows)] * heads, axis=0)
        row_c = lax.broadcasted_iota(i32, (tall, rows * slots), 0) % rows
        col_c = lax.broadcasted_iota(i32, (tall, rows * slots), 1)
        live_c = (col_c // slots == row_c) & (col_c % slots < lens)
        row_n = lax.broadcasted_iota(i32, (tall, HEAD_DIM), 0) % rows
        col_n = lax.broadcasted_iota(i32, (tall, HEAD_DIM), 1)

        def decode_a(step):
            total = jnp.zeros((rows, 1), f32)
            for q in range(feats):
                cell = st[q].astype(f32)
                total = total + jnp.sum(cell * cell, axis=1, keepdims=True)
            inv = lax.rsqrt(total / dim + 1e-06)
            for q in range(feats):
                nsend[step, q] = (
                    st[q].astype(f32) * inv * gain_w[:, q * wide : (q + 1) * wide]
                ).astype(bf)
            nbuf[step, me_d] = nsend[step, pl.ds(me_d * per, per)]
            return sent(
                nsend.at[step, pl.ds(other * per, per)],
                nbuf.at[step, me_d],
                hs.at[step],
                hr.at[step],
                to_x,
            )

        def decode_b(step):
            parts = []
            for w in (wq, wk, wv):
                acc = None
                for q in range(per):
                    left = jnp.concatenate([nbuf[step, s, q] for s in range(shards)], axis=0)
                    one = jnp.dot(
                        left, w[q * wide : (q + 1) * wide], preferred_element_type=f32
                    )
                    acc = one if acc is None else acc + one
                parts.append(acc)
            part = jnp.concatenate(parts, axis=1)
            for s in range(shards):
                psend[step, s] = part[s * rows : (s + 1) * rows]
            pbuf[step, me_d] = psend[step, me_d]
            return sent(
                psend.at[step, other], pbuf.at[step, me_d], ps.at[step], pr.at[step], to_x
            )

        def decode_c(step):
            joined = (pbuf[step, 0] + pbuf[step, 1]).astype(bf)
            query = jnp.concatenate(
                [joined[:, h * HEAD_DIM : (h + 1) * HEAD_DIM] for h in range(heads)], axis=0
            )
            kn[step * rows : (step + 1) * rows] = joined[:, qcols : qcols + HEAD_DIM]
            vn[step * rows : (step + 1) * rows] = joined[:, qcols + HEAD_DIM :]
            score_c = lax.dot_general(query, ck[...], nt, preferred_element_type=f32) * scale
            score_n = lax.dot_general(query, kn[...], nt, preferred_element_type=f32) * scale
            expo_c = jnp.where(live_c, jnp.exp(jnp.where(live_c, score_c, 0.0)), 0.0)
            live_n = (col_n % rows == row_n) & (col_n < (step + 1) * rows)
            expo_n = jnp.where(live_n, jnp.exp(jnp.where(live_n, score_n, 0.0)), 0.0)
            denom = jnp.sum(expo_c, axis=1, keepdims=True) + jnp.sum(expo_n, axis=1, keepdims=True)
            ctx = (
                jnp.dot((expo_c / denom).astype(bf), cv[...], preferred_element_type=f32)
                + jnp.dot((expo_n / denom).astype(bf), vn[...], preferred_element_type=f32)
            ).astype(bf)
            context = jnp.concatenate(
                [ctx[h * rows : (h + 1) * rows] for h in range(heads)], axis=1
            )
            for q in range(feats):
                osend[step, q] = jnp.dot(
                    context, wo[:, q * wide : (q + 1) * wide], preferred_element_type=f32
                ).astype(bf)
            obuf[step, me_t] = osend[step, me_t]
            copies = []
            for off in range(1, feats):
                peer = lax.rem(me_t + off, feats)
                sems = os_.at[step, off - 1], or_.at[step, off - 1]
                copies.append(
                    sent(osend.at[step, peer], obuf.at[step, me_t], *sems, {"tp": peer})
                )
            return copies

        def decode_d(step):
            acc = st[me_t].astype(f32)
            for s in range(feats):
                acc = acc + obuf[step, s].astype(f32)
            snew[step, me_t] = acc.astype(bf)
            copies = []
            for off in range(1, feats):
                peer = lax.rem(me_t + off, feats)
                sems = ss.at[step, off - 1], sr.at[step, off - 1]
                mine = snew.at[step, me_t]
                copies.append(sent(mine, mine, *sems, {"tp": peer}))
            return copies

        def decode_e(step, copies):
            for copy in copies:
                copy.wait()
            for q in range(feats):
                st[q] = snew[step, q]

        def normalise(src, which, column):
            def step(i, carry):
                at = pl.ds(pl.multiple_of(i * 32, 32), 32)
                to = pl.ds(pl.multiple_of(which * tokens + i * 32, 32), 32)
                columns = pl.ds(pl.multiple_of(column * wide, wide), wide)
                nb[to, columns] = (
                    src[at, :].astype(f32) * inv_s[which, at, :1] * gain_h[me_d, :, columns]
                ).astype(bf)
                return carry

            lax.fori_loop(0, tokens // 32, step, 0)

        def project(which):
            to = pl.ds(pl.multiple_of(which * tokens, tokens), tokens)
            joint[to, :] = jnp.concatenate(
                [jnp.dot(nb[to, :], w[...], preferred_element_type=f32) for w in (wq, wk, wv)],
                axis=1,
            ).astype(bf)

        def part_of(which):
            return pl.ds(pl.multiple_of(which * share, share), share)

        def turn(which):
            at = part_of(which)
            bv[at, :] = nb[:, at].T

        def hop(item, up, h, at, first):
            where = {"grp": above if up else below}
            sems = zs.at[item, int(up), h - 1], zr.at[item, int(up), h - 1]
            if item == 0:
                src = bv.at[part_of(me_t)] if first else alln.at[at, part_of(me_t)]
                return remote(src, alln.at[at, part_of(me_t)], *sems, where)
            src = alld.at[at, me_d, item - 1]
            return remote(src, src, *sems, where)

        def leaving(h):
            for up in (True, False):
                at = me_g - h + 1 if up else me_g + h - 1
                yield up, at, (at >= 0) & (me_g + 1 < groups) if up else (at < groups) & (me_g > 0)

        def arrivals(h):
            for up in (True, False):
                at = me_g - h if up else me_g + h
                yield up, at, (at >= 0) if up else (at < groups)

        def send_hop(item, h):
            for up, at, ok in leaving(h):

                @pl.when(ok)
                def _():
                    hop(item, up, h, at, h == 1).start()

        def end_hop(item, h):
            for up, at, ok in leaving(h):

                @pl.when(ok)
                def _():
                    hop(item, up, h, at, h == 1).wait_send()

        def near(up, h, at, i):
            sems = ks.at[int(up), h - 1, i], kr.at[int(up), h - 1, i]
            ref = alln.at[at, part_of(across if i == 2 else me_t)]
            return remote(ref, ref, *sems, to_y if i == 0 else to_sib)

        def cross(up, h, at, item):
            src = alld.at[at, me_d, item - 1]
            sems = xs.at[item - 1, int(up), h - 1], xr.at[item - 1, int(up), h - 1]
            return remote(src, src, *sems, to_x)

        def take(item, h):
            for up, at, ok in arrivals(h):

                @pl.when(ok)
                def _():
                    hop(item, up, h, at, False).wait_recv()

            if h + 1 < groups:
                send_hop(item, h + 1)

        def share_out(item, h):
            for up, at, ok in arrivals(h):

                @pl.when(ok)
                def _():
                    if item == 0:
                        near(up, h, at, 0).start()
                        near(up, h, at, 1).start()
                    else:
                        cross(up, h, at, item).start()

        def got(item, h):
            take(item, h)
            share_out(item, h)

        def pass_on(h):
            for up, at, ok in arrivals(h):

                @pl.when(ok)
                def _():
                    near(up, h, at, 0).wait_recv()
                    near(up, h, at, 2).start()

        def whole(up, h, at):
            near(up, h, at, 0).wait_send()
            near(up, h, at, 1).wait()
            near(up, h, at, 2).wait()

        def per_token_of(column):
            return jnp.dot(spread, column, preferred_element_type=f32)

        def scaled(at, to):
            adv_t = per_token_of(abuf[at, 0])
            target = (per_token_of(abuf[at, 1])[:, :1] + 0.5).astype(i32) * length + slot_e
            mix = jnp.where(column_e == target, adv_t[:, :1], 0.0).astype(bf)
            flat = jnp.concatenate(
                [alld[at, s, i] for s in range(shards) for i in range(2)], axis=0
            )
            to[...] = jnp.dot(mix, flat, preferred_element_type=f32).astype(bf)

        def accumulate(first):
            def step(i, carry):
                at = pl.ds(pl.multiple_of(i * 256, 256), 256)
                one = jnp.dot(bv[at, :], ms[...], preferred_element_type=f32)
                acc[at, :] = one if first else acc[at, :] + one
                return carry

            lax.fori_loop(0, half // 256, step, 0)

        last_block = jnp.where(me_g < groups // 2, groups - 1, 0)

        def absorb(h):
            for up, at, ok in arrivals(h):

                @pl.when(ok & (at != last_block))
                def _():
                    whole(up, h, at)
                    copy = pltpu.make_async_copy(alln.at[at], bv, lsem.at[8])
                    copy.start()
                    cross(up, h, at, 1).wait()
                    cross(up, h, at, 2).wait()
                    scaled(at, ms)
                    copy.wait()
                    accumulate(False)

        first = decode_a(0)
        xsent, subs, more = [], [], []

        def cross_over(i):
            xsent[i].wait()
            at = cut_at[i]
            more.append(sent(xbuf.at[at], sibx.at[at], b_s.at[i], b_r.at[i], to_sib))

        for i, at in enumerate(cut_at):
            ysent[i].wait()
            xsent.append(sent(both.at[relay, at], xbuf.at[at], x_s.at[i], x_r.at[i], to_x))
            subs.append(sent(both.at[home, at], sibd.at[at], a_s.at[i], a_r.at[i], to_sib))
            if i >= 4:
                cross_over(i - 4)
            if i == 1:
                first.wait()
                for one in load_w:
                    one.wait()
                second = decode_b(0)
            if i == 4:
                load_o.wait()
                for one in load_k:
                    one.wait()
                second.wait()
                outs = decode_c(0)
        load_c.wait()
        quarter = tokens // 4
        cot_y = []

        def send_cot(i):
            ref = cotf.at[me_t, pl.ds(i * quarter, quarter)]
            cot_y.append(sent(ref, ref, c_s.at[i], c_r.at[i], to_y))

        send_cot(0)
        cot_a = sent(cotf.at[me_t], cotf.at[me_t], c_s.at[4], c_r.at[4], to_sib)
        for copy in stats:
            copy.wait()
        for s in range(shards):
            total = sbuf[s, 0]
            for t in range(1, feats):
                total = total + sbuf[s, t]
            scales = lax.rsqrt(total / dim + 1e-06)
            inv_s[s] = jnp.broadcast_to(scales[:1], (HEAD_DIM, tokens)).T

        normalise(both.at[home], me_d, core)
        for copy in outs:
            copy.wait()
        outs = decode_d(0)
        for i in range(1, 4):
            send_cot(i)
        for copy in subs:
            copy.wait()
        normalise(sibd, me_d, 1 - core)
        project(me_d)
        for i in range(pieces - 4, pieces):
            cross_over(i)
        normalise(xbuf, other, core)
        for copy in more:
            copy.wait()
        normalise(sibx, other, 1 - core)
        project(other)
        decode_e(0, outs)
        first = decode_a(1)
        jsend[...] = jnp.dot(pm[rest, :], joint[...], preferred_element_type=f32).astype(bf)
        swap = sent(jsend, jrecv, j_s.at[0], j_r.at[0], to_x)
        turn(me_t)
        send_hop(0, 1)
        for off in range(1, feats):
            turn(lax.rem(me_t + off, feats))
        first.wait()
        second = decode_b(1)
        slot_t = lax.broadcasted_iota(i32, (tokens, 1), 0) % length

        def d_context_of(q):
            columns = pl.ds(pl.multiple_of(q * wide, wide), wide)
            return lax.dot_general(cotf[q], wo[:, columns], nt, preferred_element_type=f32)

        d_context = d_context_of(me_t)
        cot_a.wait()
        d_context = d_context + d_context_of(sib)
        cot_b = []
        for i in range(4):
            cot_y[i].wait()
            ref = cotf.at[across, pl.ds(i * quarter, quarter)]
            cot_b.append(sent(ref, ref, c_s.at[5 + i], c_r.at[5 + i], to_sib))
        d_context = d_context + d_context_of(across)
        for copy in cot_b:
            copy.wait()
        d_context = d_context + d_context_of(across + 1 - 2 * core)
        d_context = jnp.where(slot_t < count_t, d_context, 0.0).astype(bf)
        own = jnp.dot(pm[pick, :], joint[...], preferred_element_type=f32)
        swap.wait()
        joined = (own + jrecv[...].astype(f32)).astype(bf)
        keys = joined[:, qcols : qcols + HEAD_DIM]
        values = joined[:, qcols + HEAD_DIM :]
        at_i = lax.broadcasted_iota(i32, (tokens, tokens), 0)
        at_j = lax.broadcasted_iota(i32, (tokens, tokens), 1)
        mask = (at_i // length == at_j // length) & (at_j <= at_i) & (at_j % length < count_t)
        for h in range(heads):
            cols = slice(h * HEAD_DIM, (h + 1) * HEAD_DIM)
            lines = slice(h * tokens, (h + 1) * tokens)
            query, d_ctx = joined[:, cols], d_context[:, cols]
            score = lax.dot_general(query, keys, nt, preferred_element_type=f32) * scale
            expo = jnp.where(mask, jnp.exp(jnp.where(mask, score, 0.0)), 0.0)
            soft = expo / jnp.sum(expo, axis=1, keepdims=True)
            short = soft.astype(bf)
            ctx_s[:, cols] = jnp.dot(short, values, preferred_element_type=f32).astype(bf)
            d_soft = lax.dot_general(d_ctx, values, nt, preferred_element_type=f32)
            d_score = soft * (d_soft - jnp.sum(d_soft * soft, axis=1, keepdims=True)) * scale
            d_score = d_score.astype(bf)
            d_q = jnp.dot(d_score, keys, preferred_element_type=f32).astype(bf)
            for i in range(2):
                alld[me_g, me_d, i, :, cols] = d_q[i * part_rows : (i + 1) * part_rows]
            qs[lines], dcs[lines], ws[lines], dss[lines] = query, d_ctx, short, d_score
            if h == 0:
                second.wait()
                outs = decode_c(1)
            if h == heads - 2:
                take(0, 1)
                for copy in outs:
                    copy.wait()
                outs = decode_d(1)
                share_out(0, 1)
        d_k = lax.dot_general(dss[...], qs[...], tn, preferred_element_type=f32).astype(bf)
        d_v = lax.dot_general(ws[...], dcs[...], tn, preferred_element_type=f32).astype(bf)
        for i in range(2):
            lines = slice(i * part_rows, (i + 1) * part_rows)
            alld[me_g, me_d, i, :, qcols : qcols + HEAD_DIM] = d_k[lines]
            alld[me_g, me_d, i, :, qcols + HEAD_DIM :] = d_v[lines]
        for item in (1, 2):
            send_hop(item, 1)

        own_d = [
            sent(
                alld.at[me_g, me_d, i],
                alld.at[me_g, me_d, i],
                xs.at[i, 0, groups - 1],
                xr.at[i, 0, groups - 1],
                to_x,
            )
            for i in range(2)
        ]
        for q in range(feats):
            pt[q] = jnp.dot(
                ctx_s[...], wo[:, q * wide : (q + 1) * wide], preferred_element_type=f32
            ).astype(bf)
        swaps = [
            sent(pt.at[2 * s + 1 - core], sibp.at[s], ls.at[s], lr.at[s], to_sib)
            for s in range(feats // 2)
        ]
        decode_e(1, outs)
        reward = jnp.zeros((rows, 1), f32)
        for q in range(feats):
            dec_o[:, q * wide : (q + 1) * wide] = st[q]
            reward = reward + jnp.sum(
                st[q].astype(f32) * rvec[:, q * wide : (q + 1) * wide], axis=1, keepdims=True
            )
        rbuf[me_d] = jnp.broadcast_to(reward, (rows, HEAD_DIM))
        swap_r = sent(rbuf.at[me_d], rbuf.at[me_d], rs.at[0], rr.at[0], to_x)
        mine = sent(both.at[0], mbuf, j_s.at[1], j_r.at[1], to_x)
        for copy in swaps:
            copy.wait()
        theirs = lax.rem(me_t // 2 + 1, 2)
        ysend[...] = (
            pt[2 * theirs + core].astype(f32) + sibp[theirs].astype(f32)
        ).astype(bf)
        swap_y = sent(ysend, yrecv, ls.at[2], lr.at[2], to_y)
        swap_r.wait()
        every_r = jnp.concatenate([rbuf[s] for s in range(shards)], axis=0)
        mean = jnp.sum(every_r, axis=0, keepdims=True) / count
        spread_r = jnp.sum(every_r * every_r, axis=0, keepdims=True) / count - mean * mean
        adv = (every_r - mean) / jnp.sqrt(spread_r + 1e-05)
        abuf[me_g, 0] = adv.astype(bf)
        abuf[me_g, 1] = jnp.broadcast_to(place.astype(f32), (count, HEAD_DIM)).astype(bf)
        advs = []
        for off in range(1, groups):
            peer = {"grp": lax.rem(me_g + off, groups)}
            advs.append(
                sent(abuf.at[me_g], abuf.at[me_g], gs.at[off - 1], gr.at[off - 1], peer)
            )
        flat_i = lax.broadcasted_iota(i32, (count, count), 0)
        flat_j = lax.broadcasted_iota(i32, (count, count), 1)
        line = jnp.sum(
            jnp.where(flat_i == flat_j, jnp.broadcast_to(adv[:, :1], (count, count)), 0.0),
            axis=0,
            keepdims=True,
        )
        adv_o[...] = line
        for copy in own_d:
            copy.wait()
        scaled(me_g, ms)
        accumulate(True)
        got(0, 2)
        end_hop(0, 1)
        got(1, 1)
        got(2, 1)
        pass_on(1)
        got(0, 3)
        for copy in advs:
            copy.wait()
        absorb(1)
        got(1, 2)
        got(2, 2)
        pass_on(2)
        mine.wait()
        swap_y.wait()
        layer_o[...] = (
            jnp.dot(pm[pick, pick], both[0], preferred_element_type=f32)
            + jnp.dot(pm[pick, rest], mbuf[...], preferred_element_type=f32)
            + pt[me_t].astype(f32)
            + sibp[me_t // 2].astype(f32)
            + yrecv[...].astype(f32)
        ).astype(bf)
        got(1, 3)
        absorb(2)
        keep = local(acc, acc_o, 9)
        got(2, 3)
        pass_on(3)
        for h in (groups - 2, groups - 1):
            for up, at, ok in arrivals(h):

                @pl.when(ok & (at == last_block))
                def _():
                    cross(up, h, at, 1).wait()
                    cross(up, h, at, 2).wait()
                    scaled(at, dsc_o)
                    whole(up, h, at)

        keep.wait()
        for h in range(1, groups):
            for item in range(3):
                if (item, h) != (0, 1):
                    end_hop(item, h)

    dma = pltpu.SemaphoreType.DMA
    vmem, hbm = pl.BlockSpec(memory_space=pltpu.VMEM), pl.BlockSpec(memory_space=pl.ANY)

    def room(*shape, kind=bf):
        return pltpu.VMEM(shape, kind)

    return pl.pallas_call(
        kernel,
        out_shape=[
            jax.ShapeDtypeStruct((rows, dim), bf),
            jax.ShapeDtypeStruct((1, count), f32),
            jax.ShapeDtypeStruct((tokens, wide), bf),
            jax.ShapeDtypeStruct((every, join), bf),
            jax.ShapeDtypeStruct((half, join), f32),
            jax.ShapeDtypeStruct((groups, half, every), bf),
        ],
        in_specs=[vmem] * 7 + [hbm] * 8,
        out_specs=[vmem] * 4 + [hbm] * 2,
        scratch_shapes=[
            room(*weights[0].shape),
            room(*weights[1].shape),
            room(*weights[2].shape),
            room(*w_out.shape),
            room(rows * slots, HEAD_DIM),
            room(rows * slots, HEAD_DIM),
            room(2, tokens, wide),
            room(tokens, wide),
            room(tokens, wide),
            room(tokens, wide),
            room(tokens, wide),
            room(feats, tokens, wide),
            room(shards, feats, 8, tokens, kind=f32),
            room(shards, tokens, HEAD_DIM, kind=f32),
            room(every, half),
            room(half, every),
            room(every, every),
            room(every, join),
            room(tokens, join),
            room(tokens, join),
            room(deep, HEAD_DIM),
            room(deep, HEAD_DIM),
            room(deep, tokens),
            room(deep, tokens),
            room(tokens, qcols),
            room(groups, shards, 2, part_rows, join),
            room(feats, tokens, wide),
            room(feats // 2, tokens, wide),
            room(tokens, wide),
            room(tokens, wide),
            room(groups, 2, count, HEAD_DIM),
            room(half, join, kind=f32),
            room(every, join),
            room(feats, rows, wide),
            room(STEPS, feats, rows, wide),
            room(STEPS, shards, per, rows, wide),
            room(STEPS, shards, rows, join, kind=f32),
            room(STEPS, shards, rows, join, kind=f32),
            room(STEPS, feats, rows, wide),
            room(STEPS, feats, rows, wide),
            room(STEPS, feats, rows, wide),
            room(HEAD_DIM, HEAD_DIM),
            room(HEAD_DIM, HEAD_DIM),
            room(shards, rows, HEAD_DIM, kind=f32),
            dma((10,)),
            dma((shards * feats - 1,)),
            dma((shards * feats - 1,)),
        ]
        + [dma((pieces,))] * 8
        + [dma((9,)), dma((9,)), dma((2,)), dma((2,))]
        + [dma((STEPS,))] * 4
        + [dma((STEPS, feats - 1))] * 4
        + [dma((1,))] * 2
        + [dma((3, 2, groups - 1))] * 2
        + [dma((2, groups - 1, 3))] * 2
        + [dma((2, 2, groups))] * 2
        + [dma((3,))] * 2
        + [dma((groups - 1,))] * 2,
        compiler_params=pltpu.CompilerParams(
            collective_id=0, has_side_effects=True, vmem_limit_bytes=62 * 2**20
        ),
        cost_estimate=pl.CostEstimate(
            flops=40_000_000_000, bytes_accessed=2 * (join + qcols) * half, transcendentals=0
        ),
        name="main",
    )(
        hidden,
        gain.reshape(shards, 1, half),
        gain.reshape(1, -1),
        lengths.reshape(1, -1),
        reward_vec.reshape(1, -1),
        assignment.reshape(1, -1),
        response_counts.reshape(1, -1),
        own_x,
        own_cot,
        *weights,
        w_out,
        cache_keys.reshape(rows * slots, -1),
        cache_values.reshape(rows * slots, -1),
    )


def gradients(blocks, scaled, done, which, weights):
    _, half, every = blocks.shape
    join = scaled.shape[-1]
    cuts = [w.shape[1] for w in weights]
    tile = 512

    def kernel(_, n_r, d_r, a_r, q_o, k_o, v_o):
        total = a_r[...] + jnp.dot(n_r[0], d_r[...], preferred_element_type=jnp.float32)
        q_o[...] = total[:, : cuts[0]]
        k_o[...] = total[:, cuts[0] : cuts[0] + cuts[1]]
        v_o[...] = total[:, cuts[0] + cuts[1] :]

    return pl.pallas_call(
        kernel,
        out_shape=[jax.ShapeDtypeStruct((half, cut), jnp.float32) for cut in cuts],
        grid_spec=pltpu.PrefetchScalarGridSpec(
            num_scalar_prefetch=1,
            grid=(half // tile,),
            in_specs=[
                pl.BlockSpec((1, tile, every), lambda i, at: (at[0], i, 0)),
                pl.BlockSpec((every, join), lambda i, at: (0, 0)),
                pl.BlockSpec((tile, join), lambda i, at: (i, 0)),
            ],
            out_specs=[pl.BlockSpec((tile, cut), lambda i, at: (i, 0)) for cut in cuts],
        ),
        compiler_params=pltpu.CompilerParams(dimension_semantics=("arbitrary",)),
        cost_estimate=pl.CostEstimate(
            flops=2 * every * half * join,
            bytes_accessed=2 * every * (half + join) + 8 * half * join,
            transcendentals=0,
        ),
        name="gradients",
    )(which, blocks, scaled, done)


def on_device(
    hidden_last,
    gain,
    w_query,
    w_key,
    w_value,
    w_out,
    cache_keys,
    cache_values,
    cache_lengths,
    reward_vec,
    response_counts,
    assignment,
    responses,
    cotangent,
):
    rows_dev, length, _ = responses.shape
    tokens = rows_dev * length
    weights = (w_query, w_key, w_value)
    state, every_adv, layer, scaled, done, blocks = main_kernel(
        length,
        responses.reshape(tokens, -1),
        cotangent.reshape(tokens, -1),
        gain,
        weights,
        w_out,
        hidden_last,
        cache_keys,
        cache_values,
        cache_lengths,
        reward_vec,
        assignment,
        response_counts,
    )
    advantage = lax.dynamic_slice_in_dim(
        every_adv.reshape(-1), lax.axis_index("dp") * rows_dev, rows_dev
    )
    groups = lax.axis_size("grp")
    which = jnp.where(lax.axis_index("grp") < groups // 2, groups - 1, 0)
    grads = gradients(blocks, scaled, done, which.astype(jnp.int32).reshape(1), weights)
    return (state, advantage, layer.reshape(rows_dev, length, -1), *grads)


def solution(mesh):
    small = mesh.shape["grp"] == 4 and mesh.shape["dp"] == 2 and mesh.shape["tp"] == 4
    return jax.shard_map(
        on_device if small else on_device_plain,
        mesh=mesh,
        in_specs=(
            P(("grp", "dp"), None),
            P(),
            P("dp", "tp"),
            P("dp", "tp"),
            P("dp", "tp"),
            P("tp", None),
            P(("grp", "dp"), None, "tp"),
            P(("grp", "dp"), None, "tp"),
            P(("grp", "dp")),
            P(),
            P("grp"),
            P("grp"),
            P(("grp", "dp"), None, "tp"),
            P(("grp", "dp"), None, "tp"),
        ),
        out_specs=(
            P(("grp", "dp"), None),
            P(("grp", "dp")),
            P(("grp", "dp"), None, "tp"),
            P("dp", "tp"),
            P("dp", "tp"),
            P("dp", "tp"),
        ),
        check_vma=False,
    )
```

```python
import jax
import jax.numpy as jnp
from jax import lax
from jax.experimental import pallas as pl
from jax.experimental.pallas import tpu as pltpu
from jax.sharding import PartitionSpec as P

HEAD_DIM = 128
STEPS = 2
MESH = pl.DeviceIdType.MESH


def norm_rows(values, gain):
    wide = values.astype(jnp.float32)
    meansq = jnp.mean(wide * wide, axis=-1, keepdims=True)
    return (wide * lax.rsqrt(meansq + 1e-06) * gain).astype(jnp.bfloat16)


def rounded(values):
    return lax.optimization_barrier(values.astype(jnp.bfloat16)).astype(jnp.float32)


def decode_attend(query, cache_k, cache_v, lengths, new_k, new_v):
    rows_n = query.shape[0]
    slots = cache_k.shape[1]
    kv_n = cache_k.shape[2] // HEAD_DIM
    per_kv = query.shape[1] // cache_k.shape[2]
    scale = 1.0 / HEAD_DIM**0.5
    quer = query.reshape(rows_n, kv_n, per_kv, HEAD_DIM)
    keys_c = cache_k.reshape(rows_n, slots, kv_n, HEAD_DIM)
    vals_c = cache_v.reshape(rows_n, slots, kv_n, HEAD_DIM)
    keys_n = new_k.reshape(rows_n, -1, kv_n, HEAD_DIM)
    vals_n = new_v.reshape(rows_n, -1, kv_n, HEAD_DIM)
    score_c = (
        jnp.einsum("rkgd,rckd->rkgc", quer, keys_c, preferred_element_type=jnp.float32) * scale
    )
    score_n = (
        jnp.einsum("rkgd,rnkd->rkgn", quer, keys_n, preferred_element_type=jnp.float32) * scale
    )
    live = (jnp.arange(slots, dtype=jnp.int32)[None, :] < lengths[:, None])[:, None, None, :]
    score_c = jnp.where(live, score_c, -1e30)
    scores = jnp.concatenate([score_c, score_n], axis=-1)
    expo = jnp.exp(scores)
    weights = (expo / jnp.sum(expo, axis=-1, keepdims=True)).astype(jnp.bfloat16)
    context = jnp.einsum(
        "rkgc,rckd->rkgd", weights[..., :slots], vals_c, preferred_element_type=jnp.float32
    )
    context = context + jnp.einsum(
        "rkgn,rnkd->rkgd", weights[..., slots:], vals_n, preferred_element_type=jnp.float32
    )
    return context.reshape(rows_n, -1).astype(jnp.bfloat16)


def attend(query, keys, values, counts):
    rows_n = counts.shape[0]
    tokens = query.shape[0]
    length = tokens // rows_n
    kv_n = keys.shape[1] // HEAD_DIM
    per_kv = query.shape[1] // keys.shape[1]
    scale = 1.0 / HEAD_DIM**0.5
    quer = query.reshape(rows_n, length, kv_n, per_kv, HEAD_DIM).astype(jnp.float32)
    keyf = keys.reshape(rows_n, length, kv_n, HEAD_DIM).astype(jnp.float32)
    valf = values.reshape(rows_n, length, kv_n, HEAD_DIM).astype(jnp.float32)
    scores = jnp.einsum("rikgd,rjkd->rkgij", quer, keyf) * scale
    slot = jnp.arange(length, dtype=jnp.int32)
    causal = (slot[None, :] <= slot[:, None])[None, :, :]
    inside = slot[None, None, :] < counts[:, None, None]
    mask = (causal & inside)[:, None, None, :, :]
    scores = jnp.where(mask, scores, -1e30)
    expo = jnp.exp(scores)
    weights = (
        (expo / jnp.sum(expo, axis=-1, keepdims=True)).astype(jnp.bfloat16).astype(jnp.float32)
    )
    context = jnp.einsum("rkgij,rjkd->rikgd", weights, valf)
    return context.reshape(tokens, -1).astype(jnp.bfloat16)


def slot_valid(counts, length):
    slot = jnp.arange(length, dtype=jnp.int32)
    return (slot[None, :] < counts[:, None]).reshape(-1)


def exclusive_rank(labels, classes):
    onehot = (labels[:, None] == jnp.arange(classes, dtype=jnp.int32)[None, :]).astype(jnp.int32)
    return jnp.sum((jnp.cumsum(onehot, axis=0) - onehot) * onehot, axis=1)


def exchange(axis, ident, gathers=(), swaps=()):
    members = lax.axis_size(axis)
    items = tuple(gathers) + tuple(swaps)
    total = len(items)

    def kernel(*refs):
        ins, outs = refs[:total], refs[total : 2 * total]
        send_sem, recv_sem, own_sem = refs[2 * total :]
        me = lax.axis_index(axis)
        peers = [lax.rem(me + off, members) for off in range(1, members)]
        barrier = pltpu.get_barrier_semaphore()
        for peer in peers:
            pl.semaphore_signal(
                barrier, inc=1, device_id={axis: peer}, device_id_type=pl.DeviceIdType.MESH
            )
        pl.semaphore_wait(barrier, members - 1)
        copies = []
        for at, peer in enumerate(peers):
            for which in range(total):
                source = ins[which] if which < len(gathers) else ins[which].at[peer]
                copy = pltpu.make_async_remote_copy(
                    src_ref=source,
                    dst_ref=outs[which].at[me],
                    send_sem=send_sem.at[which * (members - 1) + at],
                    recv_sem=recv_sem.at[which * (members - 1) + at],
                    device_id={axis: peer},
                    device_id_type=pl.DeviceIdType.MESH,
                )
                copy.start()
                copies.append(copy)
        for which in range(total):
            source = ins[which] if which < len(gathers) else ins[which].at[me]
            copy = pltpu.make_async_copy(source, outs[which].at[me], own_sem.at[which])
            copy.start()
            copies.append(copy)
        for copy in copies:
            copy.wait()

    shapes = [(members,) + item.shape for item in gathers] + [item.shape for item in swaps]
    sent = sum(
        2 * item.size * (members if at < len(gathers) else 1) for at, item in enumerate(items)
    )
    return pl.pallas_call(
        kernel,
        out_shape=[jax.ShapeDtypeStruct(sh, item.dtype) for sh, item in zip(shapes, items)],
        in_specs=[pl.BlockSpec(memory_space=pltpu.VMEM)] * total,
        out_specs=[pl.BlockSpec(memory_space=pltpu.VMEM)] * total,
        scratch_shapes=[
            pltpu.SemaphoreType.DMA((total * (members - 1),)),
            pltpu.SemaphoreType.DMA((total * (members - 1),)),
            pltpu.SemaphoreType.DMA((total,)),
        ],
        compiler_params=pltpu.CompilerParams(collective_id=ident, has_side_effects=True),
        cost_estimate=pl.CostEstimate(
            flops=sent * 1000, bytes_accessed=2 * sent, transcendentals=0
        ),
        name=f"exchange_{ident}",
    )(*items)


def side_by_side(parts):
    return jnp.moveaxis(parts, 0, 1).reshape(parts.shape[1], -1)


def cut(values, members):
    return jnp.moveaxis(values.reshape(values.shape[0], members, -1), 1, 0)


def project(rows, weights):
    return jnp.concatenate(
        [jnp.dot(rows, weight, preferred_element_type=jnp.float32) for weight in weights], axis=1
    )


def split_qkv(joined, weights):
    first = weights[0].shape[1]
    second = first + weights[1].shape[1]
    return joined[:, :first], joined[:, first:second], joined[:, second:]


def on_device_plain(
    hidden_last,
    gain,
    w_query,
    w_key,
    w_value,
    w_out,
    cache_keys,
    cache_values,
    cache_lengths,
    reward_vec,
    response_counts,
    assignment,
    responses,
    cotangent,
):
    shards = lax.axis_size("dp")
    feats = lax.axis_size("tp")
    myself = lax.axis_index("dp")
    weights = (w_query, w_key, w_value)
    rows_dev, length, _ = responses.shape
    tokens = rows_dev * length
    group_rows = assignment.shape[0]

    positions = jnp.arange(group_rows, dtype=jnp.int32)
    place = assignment * rows_dev + exclusive_rank(assignment, shards)
    order = jnp.sum(jnp.where(place[None, :] == positions[:, None], positions[None, :], 0), axis=1)
    chosen = lax.dynamic_slice_in_dim(order, myself * rows_dev, rows_dev)

    (row_parts,) = exchange("tp", 0, gathers=(responses.reshape(tokens, -1),))
    own_normed = norm_rows(side_by_side(row_parts), gain)
    (block,) = exchange("dp", 1, swaps=(cut(own_normed, shards),))
    width = block.shape[-1]
    block = jnp.take(block.reshape(group_rows, length, width), order, axis=0)
    block = block.reshape(group_rows * length, width)
    share = group_rows * length // feats
    every_block = lax.all_gather(
        lax.dynamic_slice_in_dim(block, lax.axis_index("tp") * share, share),
        ("grp", "tp"),
        axis=0,
        tiled=True,
    )

    joined = project(block, weights).astype(jnp.bfloat16)
    mine_x = jnp.take(
        lax.all_gather(responses, "dp", axis=0, tiled=True), chosen, axis=0
    ).reshape(tokens, -1)
    (joined_parts,) = exchange("dp", 2, swaps=(joined.reshape(shards, tokens, -1),))
    joined = jnp.sum(joined_parts.astype(jnp.float32), axis=0).astype(jnp.bfloat16)
    query, keys, values = split_qkv(joined, weights)
    counts = jnp.take(response_counts, chosen)
    valid = slot_valid(counts, length)
    context, pull = jax.vjp(lambda a, b, c: attend(a, b, c, counts), query, keys, values)
    partial_out = jnp.dot(context, w_out, preferred_element_type=jnp.float32)
    layer = (
        mine_x.astype(jnp.float32)
        + lax.psum_scatter(
            partial_out.astype(jnp.bfloat16), "tp", scatter_dimension=1, tiled=True
        ).astype(jnp.float32)
    ).astype(jnp.bfloat16)

    local_cot = cotangent.reshape(tokens, -1) * valid.astype(jnp.bfloat16)[:, None]
    (cot_parts,) = exchange("tp", 3, gathers=(local_cot,))
    d_context = lax.dot_general(
        side_by_side(cot_parts),
        w_out,
        (((1,), (1,)), ((), ())),
        preferred_element_type=jnp.float32,
    ).astype(jnp.bfloat16)
    d_joined = jnp.concatenate(pull(d_context), axis=1)

    state = hidden_last
    keys_new = []
    values_new = []
    for step in range(STEPS):
        normed = norm_rows(state, gain)
        (pieces,) = exchange("dp", 4 + 3 * step, swaps=(cut(normed, shards),))
        part = project(pieces.reshape(group_rows, -1), weights)
        (parts,) = exchange("dp", 5 + 3 * step, swaps=(part.reshape(shards, rows_dev, -1),))
        step_q, step_k, step_v = split_qkv(
            jnp.sum(parts, axis=0).astype(jnp.bfloat16), weights
        )
        keys_new.append(step_k)
        values_new.append(step_v)
        step_context = decode_attend(
            step_q,
            cache_keys,
            cache_values,
            cache_lengths,
            jnp.stack(keys_new, 1),
            jnp.stack(values_new, 1),
        )
        step_out = jnp.dot(step_context, w_out, preferred_element_type=jnp.float32)
        (outs,) = exchange("tp", 6 + 3 * step, gathers=(step_out.astype(jnp.bfloat16),))
        state = (
            state.astype(jnp.float32) + jnp.sum(outs.astype(jnp.float32), axis=0)
        ).astype(jnp.bfloat16)
    reward = jnp.sum(state.astype(jnp.float32) * reward_vec, axis=-1, keepdims=True)
    (every_reward,) = exchange(
        "dp", 4 + 3 * STEPS, gathers=(jnp.broadcast_to(reward, (rows_dev, HEAD_DIM)),)
    )
    rewards = every_reward[:, :, 0].reshape(-1)
    mean = jnp.sum(rewards) / group_rows
    spread = jnp.sum(rewards * rewards) / group_rows - mean * mean
    every_adv = (rewards - mean) / jnp.sqrt(spread + 1e-05)
    advantage = lax.dynamic_slice_in_dim(every_adv, myself * rows_dev, rows_dev)
    my_adv = jnp.take(every_adv.astype(jnp.bfloat16), chosen).astype(jnp.float32)

    scaled = (jnp.repeat(my_adv, length)[:, None] * d_joined.astype(jnp.float32)).astype(
        jnp.bfloat16
    )
    every_d = lax.all_gather(scaled, ("grp", "dp"), axis=0, tiled=True)
    grad_q, grad_k, grad_v = (
        lax.dot_general(
            every_block, piece, (((0,), (0,)), ((), ())), preferred_element_type=jnp.float32
        )
        for piece in split_qkv(every_d, weights)
    )
    return (state, advantage, layer.reshape(rows_dev, length, -1), grad_q, grad_k, grad_v)


def main_kernel(
    length, own_x, own_cot, gain, weights, w_out, hidden, cache_keys, cache_values,
    lengths, reward_vec, assignment, response_counts,
):
    groups, shards, feats = lax.axis_size("grp"), lax.axis_size("dp"), lax.axis_size("tp")
    tokens, wide = own_x.shape
    half = weights[0].shape[0]
    every = shards * tokens
    heads = weights[0].shape[1] // HEAD_DIM
    qcols = weights[0].shape[1]
    join = sum(w.shape[1] for w in weights)
    rows, dim = hidden.shape
    count = shards * rows
    slots = cache_keys.shape[1]
    per = feats // shards
    share = half // feats
    pieces = 16
    lag = pieces // 2
    splits = 4
    size = tokens // pieces
    part_rows = tokens // splits
    tile = half // 4
    scale = 1.0 / HEAD_DIM**0.5
    tall, deep = heads * rows, heads * tokens
    nt = (((1,), (1,)), ((), ()))
    tn = (((0,), (0,)), ((), ()))
    bf, f32, i32 = jnp.bfloat16, jnp.float32, jnp.int32

    def kernel(
        len_r, asg_r, cnt_r, hid_h, gain_i, rvec_h, x_h, cot_h, wq_h, wk_h, wv_h, wo_h, ck_h, cv_h,
        dec_o, adv_o, layer_o, dsc_o, acc_o, alln,
        wq, wk, wv, wo, ck, cv,
        both, xbuf, sibd, sibx, mbuf, cotf, sbuf, inv_s, nb, bv, pm, joint, jsend, jrecv,
        qs, dcs, ws, dss, ctx_s, alld, pt, sibp, ysend, yrecv, abuf, acc, ms, mx, hid, gain_h, rvec,
        st, nsend, nbuf, psend, pbuf, osend, obuf, snew, kn, vn, rbuf,
        lsem, s_s, s_r, y_s, y_r, x_s, x_r, a_s, a_r, b_s, b_r, c_s, c_r, j_s, j_r,
        hs, hr, ps, pr, os_, or_, ss, sr, rs, rr, zs, zr, ks, kr, xs, xr, ls, lr, gs, gr,
    ):
        me_g, me_d, me_t = lax.axis_index("grp"), lax.axis_index("dp"), lax.axis_index("tp")
        other = 1 - me_d
        core = lax.rem(me_t, 2)
        sib = me_t + 1 - 2 * core
        across = lax.rem(me_t + 2, feats)
        relay = lax.rem(me_t // 2 + me_d + 1, 2)
        home = 1 - relay
        above, below = lax.rem(me_g + 1, groups), lax.rem(me_g + groups - 1, groups)
        to_x, to_y, to_sib = {"dp": other}, {"tp": across}, {"tp": sib}

        def local(src, dst, at):
            copy = pltpu.make_async_copy(src, dst, lsem.at[at])
            copy.start()
            return copy

        def remote(src, dst, send, recv, target):
            return pltpu.make_async_remote_copy(
                src_ref=src,
                dst_ref=dst,
                send_sem=send,
                recv_sem=recv,
                device_id=target,
                device_id_type=MESH,
            )

        def sent(*args):
            copy = remote(*args)
            copy.start()
            return copy

        load_x = local(x_h, both.at[0], 0)
        load_h = [local(hid_h, hid, 11), local(gain_i, gain_h, 12)]
        load_c = local(cot_h, cotf.at[me_t], 1)
        load_w = [local(*pair, 2 + i) for i, pair in enumerate(((wq_h, wq), (wk_h, wk), (wv_h, wv)))]
        load_o = local(wo_h, wo, 5)
        load_k = [local(ck_h, ck, 6), local(cv_h, cv, 7), local(rvec_h, rvec, 10)]
        barrier = pltpu.get_barrier_semaphore()
        peers = []
        for off in range(1, shards * feats):
            at = lax.rem(me_d * feats + me_t + off, shards * feats)
            peers.append({"dp": at // feats, "tp": lax.rem(at, feats)})
        for off in range(1, groups):
            peers.append({"grp": lax.rem(me_g + off, groups)})
        for peer in peers:
            pl.semaphore_signal(barrier, inc=1, device_id=peer, device_id_type=MESH)
        pl.semaphore_wait(barrier, len(peers))
        peers = peers[: shards * feats - 1]
        load_x.wait()

        cut_at = [pl.ds(i * size, size) for i in range(pieces)]
        wide_x = both[0].astype(f32)
        square = jnp.sum(wide_x * wide_x, axis=1, keepdims=True)
        sbuf[me_d, me_t] = jnp.broadcast_to(square, (tokens, HEAD_DIM)).T[:8]
        stats = [
            sent(sbuf.at[me_d, me_t], sbuf.at[me_d, me_t], s_s.at[i], s_r.at[i], peer)
            for i, peer in enumerate(peers)
        ]
        ysent = [
            sent(both.at[0, at], both.at[1, at], y_s.at[i], y_r.at[i], to_y)
            for i, at in enumerate(cut_at)
        ]

        def upright(line, n):
            same = lax.broadcasted_iota(i32, (n, n), 0) == lax.broadcasted_iota(i32, (n, n), 1)
            return jnp.sum(jnp.where(same, line, 0), axis=1, keepdims=True)

        label = asg_r[...]
        tall_label = upright(label, count)
        row_i = lax.broadcasted_iota(i32, (count, count), 0)
        row_j = lax.broadcasted_iota(i32, (count, count), 1)
        earlier = (label == tall_label) & (row_j < row_i)
        place = tall_label * rows + jnp.sum(
            jnp.where(earlier, 1, 0), axis=1, keepdims=True
        )
        spread_i = lax.broadcasted_iota(i32, (every, count), 0) // length
        spread = (spread_i == lax.broadcasted_iota(i32, (every, count), 1)).astype(f32).astype(bf)

        def per_token(column):
            broad = jnp.broadcast_to(column.astype(f32), (count, HEAD_DIM)).astype(bf)
            return jnp.dot(spread, broad, preferred_element_type=f32)

        slot_e = lax.broadcasted_iota(i32, (every, 1), 0) % length
        at_token = (per_token(place)[:, :1] + 0.5).astype(i32) * length + slot_e
        column_e = lax.broadcasted_iota(i32, (every, every), 1)
        pm[...] = (column_e == at_token).astype(f32).T.astype(bf)
        count_e = per_token(upright(cnt_r[...], count)).astype(bf)
        pick = pl.ds(pl.multiple_of(me_d * tokens, tokens), tokens)
        rest = pl.ds(pl.multiple_of(other * tokens, tokens), tokens)
        count_t = (
            jnp.dot(pm[pick, :], count_e, preferred_element_type=f32)[:, :1] + 0.5
        ).astype(i32)

        for one in load_h:
            one.wait()
        for q in range(feats):
            st[q] = hid[:, q * wide : (q + 1) * wide]
        kn[...] = jnp.zeros_like(kn)
        vn[...] = jnp.zeros_like(vn)

        lens = jnp.concatenate([upright(len_r[...], rows)] * heads, axis=0)
        row_c = lax.broadcasted_iota(i32, (tall, rows * slots), 0) % rows
        col_c = lax.broadcasted_iota(i32, (tall, rows * slots), 1)
        live_c = (col_c // slots == row_c) & (col_c % slots < lens)
        row_n = lax.broadcasted_iota(i32, (tall, HEAD_DIM), 0) % rows
        col_n = lax.broadcasted_iota(i32, (tall, HEAD_DIM), 1)

        def decode_a(step):
            total = jnp.zeros((rows, 1), f32)
            for q in range(feats):
                cell = st[q].astype(f32)
                total = total + jnp.sum(cell * cell, axis=1, keepdims=True)
            inv = lax.rsqrt(total / dim + 1e-06)
            for q in range(feats):
                nsend[step, q] = (
                    st[q].astype(f32) * inv * gain_h[q // per, :, (q % per) * wide : (q % per + 1) * wide]
                ).astype(bf)
            nbuf[step, me_d] = nsend[step, pl.ds(me_d * per, per)]
            return sent(
                nsend.at[step, pl.ds(other * per, per)],
                nbuf.at[step, me_d],
                hs.at[step],
                hr.at[step],
                to_x,
            )

        def decode_b(step):
            parts = []
            for w in (wq, wk, wv):
                acc = None
                for q in range(per):
                    left = jnp.concatenate([nbuf[step, s, q] for s in range(shards)], axis=0)
                    one = jnp.dot(
                        left, w[q * wide : (q + 1) * wide], preferred_element_type=f32
                    )
                    acc = one if acc is None else acc + one
                parts.append(acc)
            part = jnp.concatenate(parts, axis=1)
            for s in range(shards):
                psend[step, s] = part[s * rows : (s + 1) * rows]
            pbuf[step, me_d] = psend[step, me_d]
            return sent(
                psend.at[step, other], pbuf.at[step, me_d], ps.at[step], pr.at[step], to_x
            )

        def decode_c(step):
            joined = (pbuf[step, 0] + pbuf[step, 1]).astype(bf)
            query = jnp.concatenate(
                [joined[:, h * HEAD_DIM : (h + 1) * HEAD_DIM] for h in range(heads)], axis=0
            )
            kn[step * rows : (step + 1) * rows] = joined[:, qcols : qcols + HEAD_DIM]
            vn[step * rows : (step + 1) * rows] = joined[:, qcols + HEAD_DIM :]
            score_c = lax.dot_general(query, ck[...], nt, preferred_element_type=f32) * scale
            score_n = lax.dot_general(query, kn[...], nt, preferred_element_type=f32) * scale
            expo_c = jnp.where(live_c, jnp.exp(jnp.where(live_c, score_c, 0.0)), 0.0)
            live_n = (col_n % rows == row_n) & (col_n < (step + 1) * rows)
            expo_n = jnp.where(live_n, jnp.exp(jnp.where(live_n, score_n, 0.0)), 0.0)
            denom = jnp.sum(expo_c, axis=1, keepdims=True) + jnp.sum(expo_n, axis=1, keepdims=True)
            ctx = (
                jnp.dot((expo_c / denom).astype(bf), cv[...], preferred_element_type=f32)
                + jnp.dot((expo_n / denom).astype(bf), vn[...], preferred_element_type=f32)
            ).astype(bf)
            context = jnp.concatenate(
                [ctx[h * rows : (h + 1) * rows] for h in range(heads)], axis=1
            )
            for q in range(feats):
                osend[step, q] = jnp.dot(
                    context, wo[:, q * wide : (q + 1) * wide], preferred_element_type=f32
                ).astype(bf)
            obuf[step, me_t] = osend[step, me_t]
            copies = []
            for off in range(1, feats):
                peer = lax.rem(me_t + off, feats)
                sems = os_.at[step, off - 1], or_.at[step, off - 1]
                copies.append(
                    sent(osend.at[step, peer], obuf.at[step, me_t], *sems, {"tp": peer})
                )
            return copies

        def decode_d(step):
            acc = st[me_t].astype(f32)
            for s in range(feats):
                acc = acc + obuf[step, s].astype(f32)
            snew[step, me_t] = acc.astype(bf)
            copies = []
            for off in range(1, feats):
                peer = lax.rem(me_t + off, feats)
                sems = ss.at[step, off - 1], sr.at[step, off - 1]
                mine = snew.at[step, me_t]
                copies.append(sent(mine, mine, *sems, {"tp": peer}))
            return copies

        def decode_e(step, copies):
            for copy in copies:
                copy.wait()
            for q in range(feats):
                st[q] = snew[step, q]

        def normalise(src, which, column):
            def step(i, carry):
                at = pl.ds(pl.multiple_of(i * 32, 32), 32)
                to = pl.ds(pl.multiple_of(which * tokens + i * 32, 32), 32)
                columns = pl.ds(pl.multiple_of(column * wide, wide), wide)
                nb[to, columns] = (
                    src[at, :].astype(f32) * inv_s[which, at, :1] * gain_h[me_d, :, columns]
                ).astype(bf)
                return carry

            lax.fori_loop(0, tokens // 32, step, 0)

        def project(which):
            to = pl.ds(pl.multiple_of(which * tokens, tokens), tokens)
            joint[to, :] = jnp.concatenate(
                [jnp.dot(nb[to, :], w[...], preferred_element_type=f32) for w in (wq, wk, wv)],
                axis=1,
            ).astype(bf)

        def part_of(which):
            return pl.ds(pl.multiple_of(which * share, share), share)

        def turn(which):
            at = part_of(which)
            bv[at, :] = nb[:, at].T

        def hop(item, up, h, at, first):
            where = {"grp": above if up else below}
            sems = zs.at[item, int(up), h - 1], zr.at[item, int(up), h - 1]
            if item == 0:
                src = bv.at[part_of(me_t)] if first else alln.at[at, part_of(me_t)]
                return remote(src, alln.at[at, part_of(me_t)], *sems, where)
            src = alld.at[at, me_d, item - 1]
            return remote(src, src, *sems, where)

        def leaving(h):
            for up in (True, False):
                at = me_g - h + 1 if up else me_g + h - 1
                yield up, at, (at >= 0) & (me_g + 1 < groups) if up else (at < groups) & (me_g > 0)

        def arrivals(h):
            for up in (True, False):
                at = me_g - h if up else me_g + h
                yield up, at, (at >= 0) if up else (at < groups)

        def send_hop(item, h):
            for up, at, ok in leaving(h):

                @pl.when(ok)
                def _():
                    hop(item, up, h, at, h == 1).start()

        def end_hop(item, h):
            for up, at, ok in leaving(h):

                @pl.when(ok)
                def _():
                    hop(item, up, h, at, h == 1).wait_send()

        def near(up, h, at, i):
            sems = ks.at[int(up), h - 1, i], kr.at[int(up), h - 1, i]
            ref = alln.at[at, part_of(across if i == 2 else me_t)]
            return remote(ref, ref, *sems, to_y if i == 0 else to_sib)

        def cross(up, h, at, item):
            src = alld.at[at, me_d, item - 1]
            sems = xs.at[item - 1, int(up), h - 1], xr.at[item - 1, int(up), h - 1]
            return remote(src, src, *sems, to_x)

        def take(item, h):
            for up, at, ok in arrivals(h):

                @pl.when(ok)
                def _():
                    hop(item, up, h, at, False).wait_recv()

            if h + 1 < groups:
                send_hop(item, h + 1)

        def share_out(item, h):
            for up, at, ok in arrivals(h):

                @pl.when(ok)
                def _():
                    if item == 0:
                        near(up, h, at, 0).start()
                        near(up, h, at, 1).start()
                    else:
                        cross(up, h, at, item).start()

        def got(item, h):
            take(item, h)
            share_out(item, h)

        def pass_on(h):
            for up, at, ok in arrivals(h):

                @pl.when(ok)
                def _():
                    near(up, h, at, 0).wait_recv()
                    near(up, h, at, 2).start()

        def whole(up, h, at):
            near(up, h, at, 0).wait_send()
            near(up, h, at, 1).wait()
            near(up, h, at, 2).wait()

        def per_token_of(column):
            return jnp.dot(spread, column, preferred_element_type=f32)

        def mixing(at):
            adv_t = per_token_of(abuf[at, 0])
            target = (per_token_of(abuf[at, 1])[:, :1] + 0.5).astype(i32) * length + slot_e
            mx[...] = jnp.where(column_e == target, adv_t[:, :1], 0.0).astype(bf)

        def scaled(at, to):
            flat = jnp.concatenate(
                [alld[at, s, i] for s in range(shards) for i in range(splits)], axis=0
            )
            to[...] = jnp.dot(mx[...], flat, preferred_element_type=f32).astype(bf)

        def crossed(up, h, at):
            for item in range(1, splits + 1):
                cross(up, h, at, item).wait()

        def accumulate(first):
            def step(i, carry):
                at = pl.ds(pl.multiple_of(i * tile, tile), tile)
                one = jnp.dot(bv[at, :], ms[...], preferred_element_type=f32)
                acc[at, :] = one if first else acc[at, :] + one
                return carry

            lax.fori_loop(0, half // tile, step, 0)

        last_block = jnp.where(me_g < groups // 2, groups - 1, 0)

        def absorb(h, when):
            for up, at, ok in arrivals(h):

                @pl.when(ok & when & (at != last_block))
                def _():
                    whole(up, h, at)
                    copy = pltpu.make_async_copy(alln.at[at], bv, lsem.at[8])
                    copy.start()
                    mixing(at)
                    crossed(up, h, at)
                    scaled(at, ms)
                    copy.wait()
                    accumulate(False)

        first = decode_a(0)
        xsent, subs, more = [], [], []

        def cross_over(i):
            xsent[i].wait()
            at = cut_at[i]
            more.append(sent(xbuf.at[at], sibx.at[at], b_s.at[i], b_r.at[i], to_sib))

        for i, at in enumerate(cut_at):
            ysent[i].wait()
            xsent.append(sent(both.at[relay, at], xbuf.at[at], x_s.at[i], x_r.at[i], to_x))
            subs.append(sent(both.at[home, at], sibd.at[at], a_s.at[i], a_r.at[i], to_sib))
            if i >= lag:
                cross_over(i - lag)
            if i == pieces // 4 - 1:
                first.wait()
                for one in load_w:
                    one.wait()
                second = decode_b(0)
            if i == pieces // 2 + 1:
                load_o.wait()
                for one in load_k:
                    one.wait()
                second.wait()
                outs = decode_c(0)
        load_c.wait()
        quarter = tokens // 4
        cot_y = []

        def send_cot(i):
            ref = cotf.at[me_t, pl.ds(i * quarter, quarter)]
            cot_y.append(sent(ref, ref, c_s.at[i], c_r.at[i], to_y))

        send_cot(0)
        cot_a = sent(cotf.at[me_t], cotf.at[me_t], c_s.at[4], c_r.at[4], to_sib)
        for copy in stats:
            copy.wait()
        for s in range(shards):
            total = sbuf[s, 0]
            for t in range(1, feats):
                total = total + sbuf[s, t]
            scales = lax.rsqrt(total / dim + 1e-06)
            inv_s[s] = jnp.broadcast_to(scales[:1], (HEAD_DIM, tokens)).T

        normalise(both.at[home], me_d, core)
        for copy in outs:
            copy.wait()
        outs = decode_d(0)
        for i in range(1, 4):
            send_cot(i)
        for copy in subs:
            copy.wait()
        normalise(sibd, me_d, 1 - core)
        project(me_d)
        for i in range(pieces - lag, pieces):
            cross_over(i)
        normalise(xbuf, other, core)
        for copy in more:
            copy.wait()
        normalise(sibx, other, 1 - core)
        turn(me_t)
        send_hop(0, 1)
        project(other)
        decode_e(0, outs)
        first = decode_a(1)
        jsend[...] = jnp.dot(pm[rest, :], joint[...], preferred_element_type=f32).astype(bf)
        swap = sent(jsend, jrecv, j_s.at[0], j_r.at[0], to_x)
        for off in range(1, feats):
            turn(lax.rem(me_t + off, feats))
        first.wait()
        second = decode_b(1)
        mine = sent(both.at[0], mbuf, j_s.at[1], j_r.at[1], to_x)
        slot_t = lax.broadcasted_iota(i32, (tokens, 1), 0) % length

        def d_context_of(q):
            columns = pl.ds(pl.multiple_of(q * wide, wide), wide)
            return lax.dot_general(cotf[q], wo[:, columns], nt, preferred_element_type=f32)

        d_context = d_context_of(me_t)
        cot_a.wait()
        d_context = d_context + d_context_of(sib)
        cot_b = []
        for i in range(4):
            cot_y[i].wait()
            ref = cotf.at[across, pl.ds(i * quarter, quarter)]
            cot_b.append(sent(ref, ref, c_s.at[5 + i], c_r.at[5 + i], to_sib))
        d_context = d_context + d_context_of(across)
        for copy in cot_b:
            copy.wait()
        d_context = d_context + d_context_of(across + 1 - 2 * core)
        d_context = jnp.where(slot_t < count_t, d_context, 0.0).astype(bf)
        own = jnp.dot(pm[pick, :], joint[...], preferred_element_type=f32)
        swap.wait()
        take(0, 1)
        joined = (own + jrecv[...].astype(f32)).astype(bf)
        keys = joined[:, qcols : qcols + HEAD_DIM]
        values = joined[:, qcols + HEAD_DIM :]
        at_i = lax.broadcasted_iota(i32, (tokens, tokens), 0)
        at_j = lax.broadcasted_iota(i32, (tokens, tokens), 1)
        mask = (at_i // length == at_j // length) & (at_j <= at_i) & (at_j % length < count_t)
        for h in range(heads):
            cols = slice(h * HEAD_DIM, (h + 1) * HEAD_DIM)
            lines = slice(h * tokens, (h + 1) * tokens)
            query, d_ctx = joined[:, cols], d_context[:, cols]
            score = lax.dot_general(query, keys, nt, preferred_element_type=f32) * scale
            expo = jnp.where(mask, jnp.exp(jnp.where(mask, score, 0.0)), 0.0)
            soft = expo / jnp.sum(expo, axis=1, keepdims=True)
            short = soft.astype(bf)
            ctx_s[:, cols] = jnp.dot(short, values, preferred_element_type=f32).astype(bf)
            d_soft = lax.dot_general(d_ctx, values, nt, preferred_element_type=f32)
            d_score = soft * (d_soft - jnp.sum(d_soft * soft, axis=1, keepdims=True)) * scale
            d_score = d_score.astype(bf)
            d_q = jnp.dot(d_score, keys, preferred_element_type=f32).astype(bf)
            for i in range(splits):
                alld[me_g, me_d, i, :, cols] = d_q[i * part_rows : (i + 1) * part_rows]
            qs[lines], dcs[lines], ws[lines], dss[lines] = query, d_ctx, short, d_score
            if h == 0:
                second.wait()
                outs = decode_c(1)
            if h == heads - 2:
                for copy in outs:
                    copy.wait()
                outs = decode_d(1)
                share_out(0, 1)
        d_k = lax.dot_general(dss[...], qs[...], tn, preferred_element_type=f32).astype(bf)
        d_v = lax.dot_general(ws[...], dcs[...], tn, preferred_element_type=f32).astype(bf)
        for i in range(splits):
            lines = slice(i * part_rows, (i + 1) * part_rows)
            alld[me_g, me_d, i, :, qcols : qcols + HEAD_DIM] = d_k[lines]
            alld[me_g, me_d, i, :, qcols + HEAD_DIM :] = d_v[lines]
        for item in range(1, splits + 1):
            send_hop(item, 1)

        decode_e(1, outs)
        reward = jnp.zeros((rows, 1), f32)
        for q in range(feats):
            dec_o[:, q * wide : (q + 1) * wide] = st[q]
            reward = reward + jnp.sum(
                st[q].astype(f32) * rvec[:, q * wide : (q + 1) * wide], axis=1, keepdims=True
            )
        rbuf[me_d] = jnp.broadcast_to(reward, (rows, HEAD_DIM))
        swap_r = sent(rbuf.at[me_d], rbuf.at[me_d], rs.at[0], rr.at[0], to_x)
        own_d = [
            sent(
                alld.at[me_g, me_d, i],
                alld.at[me_g, me_d, i],
                xs.at[i, 0, groups - 1],
                xr.at[i, 0, groups - 1],
                to_x,
            )
            for i in range(splits)
        ]
        for q in range(feats):
            pt[q] = jnp.dot(
                ctx_s[...], wo[:, q * wide : (q + 1) * wide], preferred_element_type=f32
            ).astype(bf)
        swaps = [
            sent(pt.at[2 * s + 1 - core], sibp.at[s], ls.at[s], lr.at[s], to_sib)
            for s in range(feats // 2)
        ]
        swap_r.wait()
        every_r = jnp.concatenate([rbuf[s] for s in range(shards)], axis=0)
        mean = jnp.sum(every_r, axis=0, keepdims=True) / count
        spread_r = jnp.sum(every_r * every_r, axis=0, keepdims=True) / count - mean * mean
        adv = (every_r - mean) / jnp.sqrt(spread_r + 1e-05)
        abuf[me_g, 0] = adv.astype(bf)
        abuf[me_g, 1] = jnp.broadcast_to(place.astype(f32), (count, HEAD_DIM)).astype(bf)
        advs = []
        for off in range(1, groups):
            peer = {"grp": lax.rem(me_g + off, groups)}
            advs.append(
                sent(abuf.at[me_g], abuf.at[me_g], gs.at[off - 1], gr.at[off - 1], peer)
            )
        mine_adv = jnp.where(me_d == 0, adv[:rows, :rows], adv[rows:, :rows])
        flat_i = lax.broadcasted_iota(i32, (rows, rows), 0)
        flat_j = lax.broadcasted_iota(i32, (rows, rows), 1)
        line = jnp.sum(jnp.where(flat_i == flat_j, mine_adv, 0.0), axis=0, keepdims=True)
        adv_o[...] = line
        for copy in swaps:
            copy.wait()
        theirs = lax.rem(me_t // 2 + 1, 2)
        ysend[...] = (
            pt[2 * theirs + core].astype(f32) + sibp[theirs].astype(f32)
        ).astype(bf)

        def send_layer(i):
            at = pl.ds(i * (tokens // 2), tokens // 2)
            return sent(ysend.at[at], yrecv.at[at], ls.at[2 + i], lr.at[2 + i], to_y)

        got(0, 2)
        swap_y = [send_layer(0)]
        end_hop(0, 1)
        mixing(me_g)
        for copy in own_d:
            copy.wait()
        for item in range(1, splits + 1):
            if item == 3:
                scaled(me_g, ms)
                accumulate(True)
            got(item, 1)
        pass_on(1)
        for copy in advs:
            copy.wait()
        outer = (me_g == 0) | (me_g == groups - 1)
        absorb(1, outer)
        got(0, 3)
        swap_y.append(send_layer(1))
        for item in range(1, splits + 1):
            got(item, 2)
        absorb(1, jnp.logical_not(outer))
        pass_on(2)
        got(1, 3)
        got(2, 3)
        absorb(2, True)
        keep = local(acc, acc_o, 9)
        got(3, 3)
        got(4, 3)
        mixing(last_block)
        pass_on(3)
        mine.wait()
        for copy in swap_y:
            copy.wait()
        layer_o[...] = (
            jnp.dot(pm[pick, pick], both[0], preferred_element_type=f32)
            + jnp.dot(pm[pick, rest], mbuf[...], preferred_element_type=f32)
            + pt[me_t].astype(f32)
            + sibp[me_t // 2].astype(f32)
            + yrecv[...].astype(f32)
        ).astype(bf)
        for h in (groups - 2, groups - 1):
            for up, at, ok in arrivals(h):

                @pl.when(ok & (at == last_block))
                def _():
                    crossed(up, h, at)
                    scaled(at, dsc_o)
                    whole(up, h, at)

        keep.wait()
        for h in range(1, groups):
            for item in range(splits + 1):
                if (item, h) != (0, 1):
                    end_hop(item, h)

    dma = pltpu.SemaphoreType.DMA
    vmem, hbm = pl.BlockSpec(memory_space=pltpu.VMEM), pl.BlockSpec(memory_space=pl.ANY)

    def room(*shape, kind=bf):
        return pltpu.VMEM(shape, kind)

    return pl.pallas_call(
        kernel,
        out_shape=[
            jax.ShapeDtypeStruct((rows, dim), bf),
            jax.ShapeDtypeStruct((1, rows), f32),
            jax.ShapeDtypeStruct((tokens, wide), bf),
            jax.ShapeDtypeStruct((every, join), bf),
            jax.ShapeDtypeStruct((half, join), f32),
            jax.ShapeDtypeStruct((groups, half, every), bf),
        ],
        in_specs=[vmem] * 3 + [hbm] * 11,
        out_specs=[vmem] * 4 + [hbm] * 2,
        scratch_shapes=[
            room(*weights[0].shape),
            room(*weights[1].shape),
            room(*weights[2].shape),
            room(*w_out.shape),
            room(rows * slots, HEAD_DIM),
            room(rows * slots, HEAD_DIM),
            room(2, tokens, wide),
            room(tokens, wide),
            room(tokens, wide),
            room(tokens, wide),
            room(tokens, wide),
            room(feats, tokens, wide),
            room(shards, feats, 8, tokens, kind=f32),
            room(shards, tokens, HEAD_DIM, kind=f32),
            room(every, half),
            room(half, every),
            room(every, every),
            room(every, join),
            room(tokens, join),
            room(tokens, join),
            room(deep, HEAD_DIM),
            room(deep, HEAD_DIM),
            room(deep, tokens),
            room(deep, tokens),
            room(tokens, qcols),
            room(groups, shards, splits, part_rows, join),
            room(feats, tokens, wide),
            room(feats // 2, tokens, wide),
            room(tokens, wide),
            room(tokens, wide),
            room(groups, 2, count, HEAD_DIM),
            room(half, join, kind=f32),
            room(every, join),
            room(every, every),
            room(rows, dim),
            room(shards, 1, half, kind=f32),
            room(1, dim, kind=f32),
            room(feats, rows, wide),
            room(STEPS, feats, rows, wide),
            room(STEPS, shards, per, rows, wide),
            room(STEPS, shards, rows, join, kind=f32),
            room(STEPS, shards, rows, join, kind=f32),
            room(STEPS, feats, rows, wide),
            room(STEPS, feats, rows, wide),
            room(STEPS, feats, rows, wide),
            room(HEAD_DIM, HEAD_DIM),
            room(HEAD_DIM, HEAD_DIM),
            room(shards, rows, HEAD_DIM, kind=f32),
            dma((13,)),
            dma((shards * feats - 1,)),
            dma((shards * feats - 1,)),
        ]
        + [dma((pieces,))] * 8
        + [dma((9,)), dma((9,)), dma((2,)), dma((2,))]
        + [dma((STEPS,))] * 4
        + [dma((STEPS, feats - 1))] * 4
        + [dma((1,))] * 2
        + [dma((splits + 1, 2, groups - 1))] * 2
        + [dma((2, groups - 1, 3))] * 2
        + [dma((splits, 2, groups))] * 2
        + [dma((4,))] * 2
        + [dma((groups - 1,))] * 2,
        compiler_params=pltpu.CompilerParams(
            collective_id=0, has_side_effects=True, vmem_limit_bytes=62 * 2**20
        ),
        cost_estimate=pl.CostEstimate(
            flops=40_000_000_000, bytes_accessed=2 * (join + qcols) * half, transcendentals=0
        ),
        name="main",
    )(
        lengths.reshape(1, -1),
        assignment.reshape(1, -1),
        response_counts.reshape(1, -1),
        hidden,
        gain.reshape(shards, 1, half),
        reward_vec.reshape(1, -1),
        own_x,
        own_cot,
        *weights,
        w_out,
        cache_keys.reshape(rows * slots, -1),
        cache_values.reshape(rows * slots, -1),
    )


def gradients(blocks, scaled, done, weights, state, advantage, layer):
    groups, half, every = blocks.shape
    join = scaled.shape[-1]
    cuts = [w.shape[1] for w in weights]
    steps = 5
    tile = half // steps

    def kernel(n_h, d_h, a_h, s_h, t_h, l_h, s_o, t_o, l_o, q_o, k_o, v_o,
               n_s, d_s, a_s, s_s, t_s, l_s, q_s, k_s, v_s, sem, out):
        me_g = lax.axis_index("grp")
        which = jnp.where(me_g < groups // 2, groups - 1, 0)
        first = [pltpu.make_async_copy(d_h, d_s, sem.at[0])]
        loads = []
        for i in range(steps):
            at = pl.ds(i * tile, tile)
            loads.append(
                (
                    pltpu.make_async_copy(n_h.at[which, at], n_s.at[at], sem.at[3 + 2 * i]),
                    pltpu.make_async_copy(a_h.at[at], a_s.at[at], sem.at[4 + 2 * i]),
                )
            )
        rest = [
            pltpu.make_async_copy(s_h, s_s, sem.at[1]),
            pltpu.make_async_copy(l_h, l_s, sem.at[2]),
            pltpu.make_async_copy(t_h, t_s, sem.at[3 + 2 * steps]),
        ]
        for copy in first + [one for pair in loads for one in pair] + rest:
            copy.start()
        first[0].wait()
        stores = []
        for i in range(steps):
            at = pl.ds(i * tile, tile)
            for copy in loads[i]:
                copy.wait()
            total = a_s[at, :] + jnp.dot(
                n_s[at, :], d_s[...], preferred_element_type=jnp.float32
            )
            edge = 0
            for j, (buf, to) in enumerate(((q_s, q_o), (k_s, k_o), (v_s, v_o))):
                buf[at, :] = total[:, edge : edge + cuts[j]]
                edge += cuts[j]
                stores.append(pltpu.make_async_copy(buf.at[at], to.at[at], out.at[3 * i + j]))
                stores[-1].start()
        for j, (load, buf, to) in enumerate((
            (rest[0], s_s, s_o), (rest[1], l_s, l_o), (rest[2], t_s, t_o)
        )):
            load.wait()
            stores.append(pltpu.make_async_copy(buf, to, out.at[3 * steps + j]))
            stores[-1].start()
        for copy in stores:
            copy.wait()

    hbm = pl.BlockSpec(memory_space=pl.ANY)
    f32 = jnp.float32
    return pl.pallas_call(
        kernel,
        out_shape=[jax.ShapeDtypeStruct(x.shape, x.dtype) for x in (state, advantage, layer)]
        + [jax.ShapeDtypeStruct((half, cut), f32) for cut in cuts],
        in_specs=[hbm] * 6,
        out_specs=[hbm] * 6,
        scratch_shapes=[
            pltpu.VMEM((half, every), blocks.dtype),
            pltpu.VMEM((every, join), scaled.dtype),
            pltpu.VMEM((half, join), f32),
            pltpu.VMEM(state.shape, state.dtype),
            pltpu.VMEM(advantage.shape, advantage.dtype),
            pltpu.VMEM(layer.shape, layer.dtype),
        ]
        + [pltpu.VMEM((half, cut), f32) for cut in cuts]
        + [
            pltpu.SemaphoreType.DMA((4 + 2 * steps,)),
            pltpu.SemaphoreType.DMA((3 + 3 * steps,)),
        ],
        compiler_params=pltpu.CompilerParams(vmem_limit_bytes=60 * 2**20),
        cost_estimate=pl.CostEstimate(
            flops=2 * every * half * join,
            bytes_accessed=2 * every * (half + join) + 8 * half * join,
            transcendentals=0,
        ),
        name="gradients",
    )(blocks, scaled, done, state, advantage, layer)


def on_device(
    hidden_last,
    gain,
    w_query,
    w_key,
    w_value,
    w_out,
    cache_keys,
    cache_values,
    cache_lengths,
    reward_vec,
    response_counts,
    assignment,
    responses,
    cotangent,
):
    rows_dev, length, _ = responses.shape
    tokens = rows_dev * length
    weights = (w_query, w_key, w_value)
    state, every_adv, layer, scaled, done, blocks = main_kernel(
        length,
        responses.reshape(tokens, -1),
        cotangent.reshape(tokens, -1),
        gain,
        weights,
        w_out,
        hidden_last,
        cache_keys,
        cache_values,
        cache_lengths,
        reward_vec,
        assignment,
        response_counts,
    )
    state, advantage, layer, *grads = gradients(
        blocks, scaled, done, weights, state, every_adv, layer
    )
    return (state, advantage.reshape(-1), layer.reshape(rows_dev, length, -1), *grads)


def solution(mesh):
    small = mesh.shape["grp"] == 4 and mesh.shape["dp"] == 2 and mesh.shape["tp"] == 4
    return jax.shard_map(
        on_device if small else on_device_plain,
        mesh=mesh,
        in_specs=(
            P(("grp", "dp"), None),
            P(),
            P("dp", "tp"),
            P("dp", "tp"),
            P("dp", "tp"),
            P("tp", None),
            P(("grp", "dp"), None, "tp"),
            P(("grp", "dp"), None, "tp"),
            P(("grp", "dp")),
            P(),
            P("grp"),
            P("grp"),
            P(("grp", "dp"), None, "tp"),
            P(("grp", "dp"), None, "tp"),
        ),
        out_specs=(
            P(("grp", "dp"), None),
            P(("grp", "dp")),
            P(("grp", "dp"), None, "tp"),
            P("dp", "tp"),
            P("dp", "tp"),
            P("dp", "tp"),
        ),
        check_vma=False,
    )
```
